256 devices in a mesh: rp: 8 (over x, z_lo), pb: 32 (over z_hi, y, core).
Axes of the slice: x: 4, y: 4, z: 8 (z_hi: 4, z_lo: 2; z = z_hi * 2 + z_lo), core: 2. Of those that a mesh axis runs over, the one named last changes fastest.
Arguments:
- wannier_g: bfloat16 [2, 1024, 32, 1152], P(None, 'rp', 'pb'), may hold values from -0.19921875 to 0.19921875
- rp_coords: int32 [3, 1024], replicated, may hold values from -8 to 8
- q_coords: int32 [3, 512], P(None, ('rp', 'pb')), may hold values from 0 to 15
- k_index: int32 [1], replicated, may hold values from 0 to 7
- k_vectors: bfloat16 [8, 2, 32, 32], replicated, may hold values from -0.75 to 0.75
- kq_vectors: bfloat16 [512, 2, 32, 32], P(('rp', 'pb')), may hold values from -0.75 to 0.75
- modes: bfloat16 [512, 2, 36, 36], P(('rp', 'pb')), may hold values from -0.75 to 0.75
Outputs:
- rotated: float32 [512, 2, 32, 1152], P(('rp', 'pb'))
The draws below stay inside these ranges and needn't reach their ends.
All inputs are finite; a program needn't handle non-finite values.
Results may differ from the reference program's by a relative error of at most 0.0054.
Values may be sent and summed in bfloat16 or wider, within the bound.
A program may use at most 64 MiB of HBM per device.

```python
import math
import jax
import jax.numpy as jnp
from jax import lax

NB = 32
NM = 36
NR = 1024
NK = 16
KB = 8
Q_DEV = 2
Q = 512
N_RP = 8
N_PB = 32


def with_ends(entries, stream_key, least, largest):
    longest = entries.shape.index(max(entries.shape))
    spots = []
    for shift in (0, 1):
        where = [jax.random.randint(jax.random.fold_in(stream_key, axis), (), 0, length) for axis, length in enumerate(entries.shape)]
        where[longest] = (where[longest] + shift) % entries.shape[longest]
        spots.append(tuple(where))
    return entries.at[spots[0]].set(least).at[spots[1]].set(largest)


def levels(own_key, dims, cuts, low, largest):
    def one(axis_at, parts):
        heights = jax.random.uniform(jax.random.fold_in(jax.random.fold_in(own_key, 6), axis_at), (parts,), jnp.float32, low / len(cuts), largest / len(cuts))
        return jnp.repeat(jnp.exp(heights), dims[axis_at] // parts).reshape((-1,) + (1,) * (len(dims) - axis_at - 1))

    factor_of = one(*cuts[0])
    for cut in cuts[1:]:
        factor_of = factor_of * one(*cut)
    return factor_of


def centred(key, extent, width, most, split=(), dtype=jnp.bfloat16):
    values = width * jax.random.normal(key, extent, jnp.float32)
    if split:
        values = values * levels(key, extent, split, -0.22, 0.18)
    return jnp.clip(values, -most, most).astype(dtype)


def setup_inputs(seed: int = 0) -> dict:
    streams_of = jax.random.split(jax.random.key(seed), 8)
    return {
        "wannier_g": centred(streams_of[0], (2, NR, NB, NB * NM), 0.03, 0.19921875, ((1, 8), (2, 32))),
        "rp_coords": with_ends(jax.random.randint(streams_of[1], (3, NR), -8, 9), jax.random.fold_in(streams_of[1], 1), -8, 8).astype(jnp.int32),
        "q_coords": with_ends(jax.random.randint(streams_of[2], (3, Q), 0, NK), jax.random.fold_in(streams_of[2], 1), 0, NK - 1).astype(jnp.int32),
        "k_index": jax.random.randint(streams_of[3], (1,), 0, KB).astype(jnp.int32),
        "k_vectors": centred(streams_of[4], (KB, 2, NB, NB), (2 * NB) ** -0.5, 0.75),
        "kq_vectors": centred(streams_of[5], (Q, 2, NB, NB), (2 * NB) ** -0.5, 0.75, ((0, 256),)),
        "modes": centred(streams_of[6], (Q, 2, NM, NM), (2 * NM) ** -0.5, 0.75, ((0, 256),)),
    }


def phases(q_rows, r_coords):
    turns = jnp.mod(jnp.sum(q_rows[:, :, None] * r_coords[:, None, :], axis=0), NK)
    angle = turns.astype(jnp.float32) * (2.0 * math.pi / NK)
    cosine = jnp.cos(angle).astype(jnp.bfloat16)
    sine = jnp.sin(angle).astype(jnp.bfloat16)
    return jnp.concatenate([cosine, -sine], axis=1), jnp.concatenate([sine, cosine], axis=1)


def rotate(fourier, mode_vecs, unit, kq_vecs):
    count = fourier.shape[0]
    field = fourier.reshape(count, 2, NB, NB, NM).astype(jnp.float32)
    e_real, e_imag = mode_vecs[:, 0], mode_vecs[:, 1]
    e_block = jnp.stack([jnp.stack([e_real, e_imag], 2), jnp.stack([-e_imag, e_real], 2)], 1).astype(jnp.float32)
    by_mode = jnp.einsum("qcmnv,qcvdu->qdmnu", field, e_block).astype(jnp.bfloat16)
    u_real, u_imag = unit[0], unit[1]
    u_block = jnp.stack([jnp.stack([u_real, u_imag], 1), jnp.stack([-u_imag, u_real], 1)], 0).astype(jnp.float32)
    by_band = jnp.einsum("qcmnu,cndj->qdmju", by_mode.astype(jnp.float32), u_block).astype(jnp.bfloat16)
    v_real, v_imag = kq_vecs[:, 0], kq_vecs[:, 1]
    v_block = jnp.stack([jnp.stack([v_real, -v_imag], 2), jnp.stack([v_imag, v_real], 2)], 1).astype(jnp.float32)
    result = jnp.einsum("qcmju,qcmdi->qdiju", by_band.astype(jnp.float32), v_block)
    return result.reshape(count, 2, NB, NB * NM)


def reference(wannier_g, rp_coords, q_coords, k_index, k_vectors, kq_vectors, modes):
    blocks = N_RP * N_PB
    right = wannier_g.reshape(2 * NR, NB * NB * NM)
    unit = lax.dynamic_index_in_dim(k_vectors, k_index[0], 0, keepdims=False)
    q_blocks = q_coords.reshape(3, blocks, Q_DEV).transpose(1, 0, 2)
    mode_blocks = modes.reshape(blocks, Q_DEV, 2, NM, NM)
    kq_blocks = kq_vectors.reshape(blocks, Q_DEV, 2, NB, NB)

    def one_block(items):
        q_rows, mode_vecs, kq_vecs = items
        left_real, left_imag = phases(q_rows, rp_coords)
        f_real = jnp.dot(left_real, right, preferred_element_type=jnp.float32).astype(jnp.bfloat16)
        f_imag = jnp.dot(left_imag, right, preferred_element_type=jnp.float32).astype(jnp.bfloat16)
        fourier = jnp.stack([f_real, f_imag], 1)
        return rotate(fourier, mode_vecs, unit, kq_vecs)

    result = lax.map(one_block, (q_blocks, mode_blocks, kq_blocks))
    return result.reshape(Q, 2, NB, NB * NM)
```

```python
import functools
import math

import jax
import jax.numpy as jnp
from jax import lax
from jax.experimental import pallas as pl
from jax.experimental.pallas import tpu as pltpu
from jax.sharding import PartitionSpec as P

MESH = pl.DeviceIdType.MESH

NK = 16


def in_blocks(x, dim, length):
    shape = x.shape
    parts = x.reshape(*shape[:dim], length, shape[dim] // length, *shape[dim + 1 :])
    return jnp.moveaxis(parts, dim, 0)


def joined_along(parts, dim):
    shape = list(parts.shape[1:])
    shape[dim] *= parts.shape[0]
    return jnp.moveaxis(parts, 0, dim).reshape(shape)


def one_exchange(x, axis, axes, splits, concats):
    sizes = [lax.axis_size(a) for a in axes]
    parts = in_blocks(x, splits[0], sizes[0])
    parts = jnp.moveaxis(in_blocks(parts, splits[1] + 1, sizes[1]), 0, 1)
    inside = parts.shape[2:]
    parts = parts.reshape(-1, *inside)
    parts = lax.all_to_all(parts, axis, split_axis=0, concat_axis=0, tiled=True)
    parts = joined_along(parts.reshape(*sizes, *inside), concats[0] + 1)
    return joined_along(parts, concats[1])


def gather_kernel(n_rp, n_pb, x_ref, o_ref, send_sem, recv_sem):
    rp, pb = lax.axis_index("rp"), lax.axis_index("pb")
    me = rp * n_pb + pb
    total = n_rp * n_pb
    barrier = pltpu.get_barrier_semaphore()

    def greet(step, carry):
        other = lax.rem(me + step, total)
        pl.semaphore_signal(
            barrier, inc=1, device_id=(other // n_pb, lax.rem(other, n_pb)), device_id_type=MESH
        )
        return carry

    lax.fori_loop(1, total, greet, 0)
    pl.semaphore_wait(barrier, total - 1)

    def push(step, carry):
        other = lax.rem(me + step, total)
        pltpu.make_async_remote_copy(
            src_ref=x_ref,
            dst_ref=o_ref.at[me],
            send_sem=send_sem,
            recv_sem=recv_sem,
            device_id=(other // n_pb, lax.rem(other, n_pb)),
            device_id_type=MESH,
        ).start()
        return carry

    lax.fori_loop(1, total, push, 0)
    rest = o_ref.at[pl.ds(0, total - 1)]
    pltpu.make_async_copy(rest, rest, recv_sem).wait()
    pltpu.make_async_copy(rest, rest, send_sem).wait()
    o_ref[me] = x_ref[...]


def gather_coords(q_coords):
    n_rp, n_pb = lax.axis_size("rp"), lax.axis_size("pb")
    own = q_coords.shape[1]
    row = jnp.pad(q_coords.reshape(1, -1), ((0, 0), (0, 128 - 3 * own)))
    gathered = pl.pallas_call(
        functools.partial(gather_kernel, n_rp, n_pb),
        name="gather_coords",
        out_shape=jax.ShapeDtypeStruct((n_rp * n_pb, 1, 128), jnp.int32),
        in_specs=[pl.BlockSpec(memory_space=pltpu.VMEM)],
        out_specs=pl.BlockSpec(memory_space=pltpu.VMEM),
        scratch_shapes=[pltpu.SemaphoreType.DMA, pltpu.SemaphoreType.DMA],
        compiler_params=pltpu.CompilerParams(collective_id=0, has_side_effects=True),
    )(row)
    coords = gathered[:, 0, : 3 * own].reshape(-1, 3, own)
    return coords.transpose(1, 0, 2).reshape(3, -1)


def phases(q_rows, r_coords):
    turns = jnp.mod(jnp.sum(q_rows[:, :, None] * r_coords[:, None, :], axis=0), NK)
    angle = turns.astype(jnp.float32) * (2.0 * math.pi / NK)
    cosine = jnp.cos(angle).astype(jnp.bfloat16)
    sine = jnp.sin(angle).astype(jnp.bfloat16)
    return (jnp.concatenate([cosine, -sine], axis=1), jnp.concatenate([sine, cosine], axis=1))


def rotate(fourier, mode_vecs, unit, kq_vecs):
    count = fourier.shape[0]
    bands = kq_vecs.shape[2]
    branches = mode_vecs.shape[2]
    field = fourier.reshape(count, 2, bands, bands, branches)
    e_real, e_imag = (mode_vecs[:, 0], mode_vecs[:, 1])
    e_block = jnp.stack([jnp.stack([e_real, e_imag], 2), jnp.stack([-e_imag, e_real], 2)], 1)
    by_mode = jnp.einsum(
        "qcmnv,qcvdu->qdmnu", field, e_block, preferred_element_type=jnp.float32
    ).astype(jnp.bfloat16)
    u_real, u_imag = (unit[0], unit[1])
    u_block = jnp.stack([jnp.stack([u_real, u_imag], 1), jnp.stack([-u_imag, u_real], 1)], 0)
    by_band = jnp.einsum(
        "qcmnu,cndj->qdmju", by_mode, u_block, preferred_element_type=jnp.float32
    ).astype(jnp.bfloat16)
    v_real, v_imag = (kq_vecs[:, 0], kq_vecs[:, 1])
    v_block = jnp.stack([jnp.stack([v_real, -v_imag], 2), jnp.stack([v_imag, v_real], 2)], 1)
    result = jnp.einsum("qcmju,qcmdi->qdiju", by_band, v_block, preferred_element_type=jnp.float32)
    return result.reshape(count, 2, bands, bands * branches)


def local(wannier_g, rp_coords, q_coords, k_index, k_vectors, kq_vectors, modes):
    q_all = gather_coords(q_coords)
    total = q_all.shape[1]
    groups = lax.axis_size("rp")
    block = total // groups
    moved = lax.all_to_all(wannier_g, "rp", split_axis=3, concat_axis=1, tiled=True)
    right = moved.reshape(2 * moved.shape[1], -1)
    q_blocks = q_all.reshape(3, groups, block).transpose(1, 0, 2)

    def fourier_block(q_rows):
        left_real, left_imag = phases(q_rows, rp_coords)
        f_real = jnp.dot(left_real, right, preferred_element_type=jnp.float32).astype(jnp.bfloat16)
        f_imag = jnp.dot(left_imag, right, preferred_element_type=jnp.float32).astype(jnp.bfloat16)
        return jnp.stack([f_real, f_imag], 1)

    fourier = lax.map(fourier_block, q_blocks).reshape(total, 2, moved.shape[2], moved.shape[3])
    owned = one_exchange(fourier, ("rp", "pb"), ("rp", "pb"), (0, 0), (3, 2))
    select = (jnp.arange(k_vectors.shape[0]) == k_index[0]).astype(jnp.bfloat16)
    unit = jnp.einsum("k,kcnj->cnj", select, k_vectors, preferred_element_type=jnp.float32).astype(
        jnp.bfloat16
    )
    return rotate(owned, modes, unit, kq_vectors)


def solution(mesh):
    return jax.shard_map(
        local,
        mesh=mesh,
        in_specs=(
            P(None, "rp", "pb", None),
            P(),
            P(None, ("rp", "pb")),
            P(),
            P(),
            P(("rp", "pb"), None, None, None),
            P(("rp", "pb"), None, None, None),
        ),
        out_specs=P(("rp", "pb"), None, None, None),
        check_vma=False,
    )
```

```python
import functools
import math

import jax
import jax.numpy as jnp
from jax import lax
from jax.experimental import pallas as pl
from jax.experimental.pallas import tpu as pltpu
from jax.sharding import PartitionSpec as P

MESH = pl.DeviceIdType.MESH
F32 = jnp.float32
BF16 = jnp.bfloat16
NK = 16
N_RP = 8
N_PB = 32
N_FAR = 4
N_NEAR = 8
N_DEV = N_RP * N_PB
NB = 32
NM = 36
COLS = NB * NM
R_DEV = 128
LANES = 128
TILES = COLS // LANES
K_ALL = 2 * R_DEV * N_RP
BANDS = tuple(
    (256 * t, min(256, COLS - 256 * t), max(0, 256 * t - 128), min(COLS, 256 * t + 384)) for t in range(5)
)


def iota(shape, dim):
    return lax.broadcasted_iota(jnp.int32, shape, dim)


def band_of(x):
    return lax.shift_right_logical(x * 1821, 16)


def dot(a, b):
    return jnp.dot(a, b, preferred_element_type=F32)


def tdot(a, b):
    return lax.dot_general(a, b, (((0,), (0,)), ((), ())), preferred_element_type=F32)


def onehot(cond):
    return jnp.where(cond, 1.0, 0.0).astype(BF16)


def kernel(
    w_hbm, rc_ref, q_ref, ki_ref, kv_ref, kq_ref, e_ref, out_ref,
    wv, wr, wr2, q1, q2, ba, ph, s1, s2, rv, vb, ku, ke, y2, z2,
    w_sem, q_send, q_recv, w_send, w_recv, f_send, f_recv,
):
    rp, pb = lax.axis_index("rp"), lax.axis_index("pb")
    far, near = pb // N_NEAR, lax.rem(pb, N_NEAR)
    y_at, core = near // 2, lax.rem(near, 2)
    hot_even = 2 * lax.rem(y_at + far, 4) + lax.rem(y_at + far // 2, 2)
    hot_odd = lax.rem(hot_even + 4, 8) + 1 - 2 * lax.rem(hot_even, 2)
    hot = jnp.where(core == 0, hot_even, hot_odd)
    is_hot = rp == hot

    load = pltpu.make_async_copy(w_hbm, wv, w_sem)
    load.start()

    rp_peers = [lax.rem(rp + d, N_RP) for d in range(1, N_RP)]
    near_peers = [far * N_NEAR + lax.rem(near + d, N_NEAR) for d in range(1, N_NEAR)]
    far_peers = [lax.rem(far + d, N_FAR) * N_NEAR + near for d in range(1, N_FAR)]
    barrier = pltpu.get_barrier_semaphore()
    for other in rp_peers:
        pl.semaphore_signal(barrier, inc=1, device_id=(other, pb), device_id_type=MESH)
    for other in near_peers + far_peers:
        pl.semaphore_signal(barrier, inc=1, device_id=(rp, other), device_id_type=MESH)

    lane, row = iota((8, LANES), 1), iota((8, LANES), 0)
    k = lane - 16 * rp
    tile = jnp.where((k == 3) & (row % 2 == 1), 12.0, 0.0) + jnp.where(k == 4, 1.0, 0.0)
    for ql in range(2):
        for axis in range(3):
            value = q_ref[ql, axis].astype(F32)
            tile = tile + jnp.where((k == axis) & (row // 2 == ql), value, 0.0)
    q1[rp] = tile[:4].astype(BF16)

    pl.semaphore_wait(barrier, (N_RP - 1) + (N_NEAR - 1) + (N_FAR - 1))

    for other in rp_peers:
        pltpu.make_async_remote_copy(
            q1.at[rp], q1.at[rp], q_send.at[0], q_recv.at[0], device_id=(other, pb), device_id_type=MESH
        ).start()
    load.wait()
    for other in rp_peers:
        columns = pl.ds(pl.multiple_of(other * LANES, LANES), LANES)
        pltpu.make_async_remote_copy(
            wv.at[:, :, columns], wr.at[rp], w_send.at[0], w_recv.at[0], device_id=(other, pb), device_id_type=MESH
        ).start()
    last = wv.at[:, :, pl.ds((TILES - 1) * LANES, LANES)]

    @pl.when(jnp.logical_not(is_hot))
    def _():
        pltpu.make_async_remote_copy(
            last, wr2.at[rp], w_send.at[1], w_recv.at[1], device_id=(hot, pb), device_id_type=MESH
        ).start()

    row = iota((16, LANES), 0)
    for p in range(N_RP):
        r_at = pl.ds(p * R_DEV, R_DEV)
        for c in range(2):
            block = jnp.where(row == 3, 1.0, 0.0) + jnp.where(row == 4, 4.0 * c, 0.0)
            for axis in range(3):
                block = block + jnp.where(row == axis, rc_ref[axis : axis + 1, r_at].astype(F32), 0.0)
            at = pl.ds((2 * p + c) * R_DEV, R_DEV)
            for g in range(N_RP):
                ba[16 * g : 16 * g + 16, at] = block.astype(BF16)

    wr[rp] = wv[:, :, pl.ds(pl.multiple_of(rp * LANES, LANES), LANES)]

    @pl.when(is_hot)
    def _():
        wr2[rp] = wv[:, :, pl.ds((TILES - 1) * LANES, LANES)]

    for ql in range(2):
        col = iota((NB, LANES), 1) - 4 * iota((NB, LANES), 0)
        place = [onehot(col == 2 * ql + c) for c in range(2)]
        v = [kq_ref[ql, c] for c in range(2)]
        top = tdot(v[0], place[0]) + tdot(v[1], place[1])
        low = tdot(v[0], place[1]) - tdot(v[1], place[0])
        at = 64 * ql
        vb[at : at + 32] = top.astype(BF16)
        vb[at + 32 : at + 64] = low.astype(BF16)
        vb[128 + at : 128 + at + 32] = (-low).astype(BF16)
        vb[128 + at + 32 : 128 + at + 64] = top.astype(BF16)

    unit = kv_ref[ki_ref[0]]
    c_col = iota((NB, COLS), 1)
    spread = onehot(band_of(c_col) == iota((NB, COLS), 0))
    uc = [dot(unit[c], spread).astype(BF16) for c in range(2)]

    def band_rows(b, carry):
        start = pl.multiple_of(b * LANES, LANES)
        r = start + iota((LANES, 1), 0)
        pick = onehot(band_of(start + iota((LANES, NB), 0)) == iota((LANES, NB), 1))
        r_mode = r - NM * band_of(r)
        col = iota((1, COLS), 1)
        same = r_mode == col - NM * band_of(col)
        for c in range(2):
            full = dot(pick, uc[c])
            ku[pl.ds(c * COLS + start, LANES), :] = jnp.where(same, full, 0.0).astype(BF16)
        return carry

    lax.fori_loop(0, COLS // LANES, band_rows, 0)

    pltpu.make_async_copy(q1.at[pl.ds(0, N_RP - 1)], q1.at[pl.ds(0, N_RP - 1)], q_recv.at[0]).wait()
    q2[pb] = jnp.sum(q1[...].astype(F32), axis=0).astype(BF16)
    for other in near_peers:
        pltpu.make_async_remote_copy(
            q2.at[pb], q2.at[pb], q_send.at[1], q_recv.at[1], device_id=(rp, other), device_id_type=MESH
        ).start()

    def branch_rows(ql):
        mode_col = iota((NM, COLS), 1)
        spread_m = onehot(mode_col - NM * band_of(mode_col) == iota((NM, COLS), 0))
        ec = [dot(e_ref[ql, c], spread_m).astype(BF16) for c in range(2)]
        for t, (c0, width, r0, r1) in enumerate(BANDS):
            rows = r1 - r0
            r = r0 + iota((rows, NM), 0)
            pick = onehot(r - NM * band_of(r) == iota((rows, NM), 1))
            same = band_of(r0 + iota((rows, 1), 0)) == band_of(c0 + iota((1, width), 1))
            for c in range(2):
                full = dot(pick, ec[c][:, c0 : c0 + width])
                ke[ql, t, c * rows : (c + 1) * rows, 0:width] = jnp.where(same, full, 0.0).astype(BF16)

    branch_rows(0)

    pltpu.make_async_copy(q2.at[pl.ds(0, N_NEAR - 1)], q2.at[pl.ds(0, N_NEAR - 1)], q_recv.at[1]).wait()
    own_far = q2.at[pl.ds(far * N_NEAR, N_NEAR)]
    for other in far_peers:
        pltpu.make_async_remote_copy(
            own_far, own_far, q_send.at[2], q_recv.at[2], device_id=(rp, other), device_id_type=MESH
        ).start()

    table = jnp.cos((iota((8, LANES), 1) % NK).astype(F32) * (2.0 * math.pi / NK))
    table = jnp.broadcast_to(table[0:1], (256, LANES))

    def fill_phases(z):
        some = q2[pl.ds(z * N_NEAR, N_NEAR)].astype(F32).reshape(4 * N_NEAR, LANES)
        group = iota((4 * N_NEAR, LANES), 1) // 16
        left = jnp.concatenate([jnp.where(group == g, some, 0.0) for g in range(N_RP)], axis=0).astype(BF16)

        def columns(p, carry):
            for c in range(2):
                at = pl.ds(pl.multiple_of((2 * p + c) * LANES, LANES), LANES)
                turns = dot(left, ba[:, at]).astype(jnp.int32) & (NK - 1)
                ph[z, :, at] = jnp.take_along_axis(table, turns, axis=1, mode="promise_in_bounds").astype(BF16)
            return carry

        lax.fori_loop(0, N_RP, columns, 0)

    fill_phases(far)
    branch_rows(1)

    pltpu.make_async_copy(
        q2.at[pl.ds(0, (N_FAR - 1) * N_NEAR)], q2.at[pl.ds(0, (N_FAR - 1) * N_NEAR)], q_recv.at[2]
    ).wait()
    for d in range(1, N_FAR):
        fill_phases(lax.rem(far + d, N_FAR))

    pltpu.make_async_copy(wr.at[pl.ds(0, N_RP - 1)], wr.at[pl.ds(0, N_RP - 1)], w_recv.at[0]).wait()

    @pl.when(is_hot)
    def _():
        pltpu.make_async_copy(wr2.at[pl.ds(0, N_RP - 1)], wr2.at[pl.ds(0, N_RP - 1)], w_recv.at[1]).wait()

    mine = rp * N_NEAR + near

    def send_plane(z, first, src, slot, sem):
        def push(step, carry):
            other = lax.rem(mine + step, N_RP * N_NEAR)
            pltpu.make_async_remote_copy(
                src.at[z, other],
                rv.at[slot],
                f_send.at[sem],
                f_recv.at[sem],
                device_id=(other // N_NEAR, z * N_NEAR + lax.rem(other, N_NEAR)),
                device_id_type=MESH,
            ).start()
            return carry

        lax.fori_loop(first, N_RP * N_NEAR, push, 0)

    for d in range(N_FAR):
        z = lax.rem(far + d, N_FAR)
        part = dot(ph[z], wr[...].reshape(K_ALL, LANES))
        s1[z] = part.astype(BF16).reshape(N_RP * N_NEAR, 4, LANES)

        @pl.when(is_hot)
        def _():
            part = dot(ph[z], wr2[...].reshape(K_ALL, LANES))
            s2[z] = part.astype(BF16).reshape(N_RP * N_NEAR, 4, LANES)

        send_plane(z, 1 if d == 0 else 0, s1, rp * N_PB + pb, 0)

        @pl.when(is_hot)
        def _():
            send_plane(z, 1 if d == 0 else 0, s2, N_RP * N_PB + pb, 1)

    rv[rp * N_PB + pb] = s1[far, mine]

    @pl.when(is_hot)
    def _():
        rv[N_RP * N_PB + pb] = s2[far, mine]

    def wait_blocks(count, sem):
        pltpu.make_async_copy(rv.at[pl.ds(0, count)], rv.at[pl.ds(0, count)], sem).wait()

    wait_blocks(N_DEV - 1, f_recv.at[0])

    @pl.when(is_hot)
    def _():
        wait_blocks(N_PB - 1, f_recv.at[1])

    @pl.when(jnp.logical_not(is_hot))
    def _():
        wait_blocks(N_PB, f_recv.at[1])

    for t in range(TILES):
        got = rv[t * N_PB : (t + 1) * N_PB].reshape(4 * N_PB, LANES)
        both = dot(vb[...], got).astype(BF16)
        y2[:, t * LANES : (t + 1) * LANES] = both[:128]
        y2[:, COLS + t * LANES : COLS + (t + 1) * LANES] = both[128:]
    for t in range(5):
        c0, width = BANDS[t][:2]
        part = dot(y2[...], ku[:, c0 : c0 + width])
        z2[0, :, c0 : c0 + width] = part.astype(BF16)
        for ql in range(2):
            at = 64 * ql
            z2[1, at : at + 32, c0 : c0 + width] = (-part[at + 32 : at + 64]).astype(BF16)
            z2[1, at + 32 : at + 64, c0 : c0 + width] = part[at : at + 32].astype(BF16)
    for ql in range(2):
        rows = slice(64 * ql, 64 * ql + 64)
        for t, (c0, width, r0, r1) in enumerate(BANDS):
            n = r1 - r0
            left = jnp.concatenate([z2[0, rows, r0:r1], z2[1, rows, r0:r1]], axis=1)
            out_ref[rows, c0 : c0 + width] = dot(left, ke[ql, t, 0 : 2 * n, 0:width])

    pltpu.make_async_copy(q1.at[pl.ds(0, N_RP - 1)], q1.at[pl.ds(0, N_RP - 1)], q_send.at[0]).wait()
    pltpu.make_async_copy(q2.at[pl.ds(0, N_NEAR - 1)], q2.at[pl.ds(0, N_NEAR - 1)], q_send.at[1]).wait()
    pltpu.make_async_copy(
        q2.at[pl.ds(0, (N_FAR - 1) * N_NEAR)], q2.at[pl.ds(0, (N_FAR - 1) * N_NEAR)], q_send.at[2]
    ).wait()
    pltpu.make_async_copy(wr.at[pl.ds(0, N_RP - 1)], wr.at[pl.ds(0, N_RP - 1)], w_send.at[0]).wait()
    wait_blocks(N_DEV - 1, f_send.at[0])

    @pl.when(is_hot)
    def _():
        wait_blocks(N_DEV - 1, f_send.at[1])

    @pl.when(jnp.logical_not(is_hot))
    def _():
        pltpu.make_async_copy(wr.at[0], wr.at[0], w_send.at[1]).wait()


def local(wannier_g, rp_coords, q_coords, k_index, k_vectors, kq_vectors, modes):
    vmem = pl.BlockSpec(memory_space=pltpu.VMEM)
    smem = pl.BlockSpec(memory_space=pltpu.SMEM)
    out = pl.pallas_call(
        kernel,
        name="wannier_to_bloch",
        out_shape=jax.ShapeDtypeStruct((4 * NB, COLS), F32),
        in_specs=[pl.BlockSpec(memory_space=pl.ANY), vmem, smem, smem, vmem, vmem, vmem],
        out_specs=vmem,
        scratch_shapes=[
            pltpu.VMEM((2, R_DEV, COLS), BF16),
            pltpu.VMEM((N_RP, 2, R_DEV, LANES), BF16),
            pltpu.VMEM((N_RP, 2, R_DEV, LANES), BF16),
            pltpu.VMEM((N_RP, 4, LANES), BF16),
            pltpu.VMEM((N_PB, 4, LANES), BF16),
            pltpu.VMEM((LANES, K_ALL), BF16),
            pltpu.VMEM((N_FAR, 4 * N_RP * N_NEAR, K_ALL), BF16),
            pltpu.VMEM((N_FAR, N_RP * N_NEAR, 4, LANES), BF16),
            pltpu.VMEM((N_FAR, N_RP * N_NEAR, 4, LANES), BF16),
            pltpu.VMEM((TILES * N_PB, 4, LANES), BF16),
            pltpu.VMEM((256, LANES), BF16),
            pltpu.VMEM((2 * COLS, COLS), BF16),
            pltpu.VMEM((2, 5, 1024, 256), BF16),
            pltpu.VMEM((128, 2 * COLS), BF16),
            pltpu.VMEM((2, 128, COLS), BF16),
            pltpu.SemaphoreType.DMA,
            pltpu.SemaphoreType.DMA((3,)),
            pltpu.SemaphoreType.DMA((3,)),
            pltpu.SemaphoreType.DMA((2,)),
            pltpu.SemaphoreType.DMA((2,)),
            pltpu.SemaphoreType.DMA((2,)),
            pltpu.SemaphoreType.DMA((2,)),
        ],
        compiler_params=pltpu.CompilerParams(
            collective_id=0, has_side_effects=True, vmem_limit_bytes=60 * 2**20
        ),
    )(wannier_g[:, :, 0, :], rp_coords, q_coords.T, k_index, k_vectors, kq_vectors, modes)
    return out.reshape(2, 2, NB, COLS)


def solution(mesh):
    return jax.shard_map(
        local,
        mesh=mesh,
        in_specs=(
            P(None, "rp", "pb", None),
            P(),
            P(None, ("rp", "pb")),
            P(),
            P(),
            P(("rp", "pb"), None, None, None),
            P(("rp", "pb"), None, None, None),
        ),
        out_specs=P(("rp", "pb"), None, None, None),
        check_vma=False,
    )
```

```python
import functools
import math

import jax
import jax.numpy as jnp
from jax import lax
from jax.experimental import pallas as pl
from jax.experimental.pallas import tpu as pltpu
from jax.sharding import PartitionSpec as P

MESH = pl.DeviceIdType.MESH
F32 = jnp.float32
BF16 = jnp.bfloat16
NK = 16
N_RP = 8
N_PB = 32
N_FAR = 4
N_NEAR = 8
NEXT = (0, 1, 3, 2)
EARLY = 2
EARLY_ROWS = 5
SINE = (6.281640231507743, -41.11355805211909, 73.72054790475445)
ROUND = 1.5 * 2.0**23
N_DEV = N_RP * N_PB
NB = 32
NM = 36
COLS = NB * NM
R_DEV = 128
LANES = 128
TILES = COLS // LANES
NR = R_DEV * N_RP
K_ALL = 2 * R_DEV * N_RP
BANDS = tuple(
    (256 * t, min(256, COLS - 256 * t), max(0, 256 * t - 128), min(COLS, 256 * t + 384)) for t in range(5)
)


def iota(shape, dim):
    return lax.broadcasted_iota(jnp.int32, shape, dim)


def band_of(x):
    return lax.shift_right_logical(x * 1821, 16)


def dot(a, b):
    return jnp.dot(a, b, preferred_element_type=F32)


def tdot(a, b):
    return lax.dot_general(a, b, (((0,), (0,)), ((), ())), preferred_element_type=F32)


def hot_rp(pb):
    far, y_at, core = pb // 8, pb % 8 // 2, pb % 2
    even = 2 * ((y_at + far) % 4) + (y_at + far // 2) % 2
    odd = (even + 4) % 8 + 1 - 2 * (even % 2)
    return even * (1 - core) + odd * core


def onehot(cond):
    return jnp.where(cond, 1.0, 0.0).astype(BF16)


def sine(c):
    c2 = c * c
    return (c * (SINE[0] + c2 * (SINE[1] + c2 * SINE[2]))).astype(BF16)


def kernel(
    w_hbm, rc_hbm, q_ref, ki_ref, kv_hbm, kq_hbm, e_hbm, out_ref,
    wv, rc, kv, kq, em, wr, wr2, wx, wx2, q1, q2, ba, ph, send, rv, vb, ku, ke, y2, z2,
    in_sem, q_send, q_recv, w_send, w_recv, f_send, f_recv,
):
    rp, pb = lax.axis_index("rp"), lax.axis_index("pb")
    hot = hot_rp(pb)
    is_hot = rp == hot
    not_hot = rp != hot
    loads = [
        pltpu.make_async_copy(src, dst, in_sem.at[i])
        for i, (src, dst) in enumerate(((w_hbm, wv), (rc_hbm, rc), (kv_hbm, kv), (kq_hbm, kq), (e_hbm, em)))
    ]
    for load in loads:
        load.start()

    rp_peers = [lax.rem(rp + d, N_RP) for d in range(1, N_RP)]
    far, near = pb // N_NEAR, lax.rem(pb, N_NEAR)
    pb_peers = [
        (d, lax.rem(far + d, N_FAR) * N_NEAR + lax.rem(near + j, N_NEAR))
        for d in NEXT
        for j in range(1 if d == 0 else 0, N_NEAR)
    ]
    barrier = pltpu.get_barrier_semaphore()
    for other in rp_peers:
        pl.semaphore_signal(barrier, inc=1, device_id=(other, pb), device_id_type=MESH)
    for _, other in pb_peers:
        pl.semaphore_signal(barrier, inc=1, device_id=(rp, other), device_id_type=MESH)

    lane, row = iota((8, LANES), 1), iota((8, LANES), 0)
    tile = jnp.zeros((8, LANES), F32)
    for ql in range(2):
        for axis in range(3):
            tile = tile + jnp.where((lane == 16 * rp + axis) & (row == ql), q_ref[ql, axis].astype(F32), 0.0)
    q1[rp] = tile[:2].astype(BF16)

    pl.semaphore_wait(barrier, (N_RP - 1) + (N_PB - 1))

    for other in rp_peers:
        pltpu.make_async_remote_copy(
            q1.at[rp], q1.at[rp], q_send.at[0], q_recv.at[0], device_id=(other, pb), device_id_type=MESH
        ).start()
    for load in loads:
        load.wait()

    def send_w(others):
        for other in others:
            columns = pl.ds(pl.multiple_of(other * LANES, LANES), LANES)
            pltpu.make_async_remote_copy(
                wv.at[:, :, columns], wr.at[rp], w_send.at[0], w_recv.at[0], device_id=(other, pb), device_id_type=MESH
            ).start()

    send_w(rp_peers[:EARLY])

    row = iota((16, NR), 0)
    block = jnp.zeros((16, NR), F32)
    for axis in range(3):
        block = block + jnp.where(row == axis, rc[axis : axis + 1, :].astype(F32) / NK, 0.0)
    for g in range(N_RP):
        ba[16 * g : 16 * g + 16, :] = block.astype(BF16)

    wr[rp] = wv[:, :, pl.ds(pl.multiple_of(rp * LANES, LANES), LANES)]

    @pl.when(is_hot)
    def _():
        wr2[rp] = wv[:, :, pl.ds((TILES - 1) * LANES, LANES)]

    for ql in range(2):
        place = onehot(iota((NB, 2 * NB), 1) - 2 * iota((NB, 2 * NB), 0) == ql)
        for c in range(2):
            at = 64 * c + 32 * ql
            vb[at : at + 32] = tdot(kq[ql, c], place).astype(BF16)

    def band_rows(b, unit):
        spread = onehot(band_of(iota((NB, COLS), 1)) == iota((NB, COLS), 0))
        pick = onehot(band_of(b * LANES + iota((LANES, NB), 0)) == iota((LANES, NB), 1))
        r = b * LANES + iota((LANES, 1), 0)
        col = iota((1, COLS), 1)
        same = r - NM * band_of(r) == col - NM * band_of(col)
        for c in range(2):
            full = dot(dot(pick, unit[c]).astype(BF16), spread)
            ku[c * COLS + b * LANES : c * COLS + (b + 1) * LANES, :] = jnp.where(same, full, 0.0).astype(BF16)

    def branch_rows(ql):
        mode_col = iota((NM, COLS), 1)
        spread_m = onehot(mode_col - NM * band_of(mode_col) == iota((NM, COLS), 0))
        ec = dot(em[ql].reshape(2 * NM, NM), spread_m).astype(BF16)
        for t, (c0, width, r0, r1) in enumerate(BANDS):
            rows = r1 - r0
            r = r0 + iota((rows, 2 * NM), 0)
            at = iota((rows, 2 * NM), 1) - 2 * (r - NM * band_of(r))
            same = band_of(r0 + iota((rows, 1), 0)) == band_of(c0 + iota((1, width), 1))
            for c in range(2):
                full = dot(onehot(at == c), ec[:, c0 : c0 + width])
                ke[ql, t, c * rows : (c + 1) * rows, 0:width] = jnp.where(same, full, 0.0).astype(BF16)

    unit = kv[ki_ref[0]]
    for b in range(EARLY_ROWS):
        band_rows(b, unit)

    rest = q1.at[pl.ds(0, N_RP - 1)]
    pltpu.make_async_copy(rest, rest, q_recv.at[0]).wait()
    q2[pb] = jnp.sum(q1[...].astype(F32), axis=0).astype(BF16)
    for d, other in pb_peers:
        pltpu.make_async_remote_copy(
            q2.at[pb], q2.at[pb], q_send.at[1], q_recv.at[1 + (N_FAR - d) % N_FAR],
            device_id=(rp, other), device_id_type=MESH,
        ).start()
    send_w(rp_peers[EARLY:])

    @pl.when(not_hot)
    def _():
        last = wv.at[:, :, pl.ds((TILES - 1) * LANES, LANES)]
        pltpu.make_async_remote_copy(
            last, wr2.at[rp], w_send.at[1], w_recv.at[1], device_id=(hot, pb), device_id_type=MESH
        ).start()

    def fill_phases(d):
        rest = q2.at[pl.ds(0, N_NEAR - (d == 0))]
        pltpu.make_async_copy(rest, rest, q_recv.at[1 + d]).wait()
        z = lax.rem(far + d, N_FAR)
        some = q2[pl.ds(z * N_NEAR, N_NEAR)].astype(F32).reshape(2 * N_NEAR, LANES)
        group = iota((2 * N_NEAR, LANES), 1) // 16
        left = jnp.concatenate([jnp.where(group == g, some, 0.0) for g in range(N_RP)], axis=0).astype(BF16)
        for p in range(N_RP):
            turns = dot(left, ba[:, p * R_DEV : (p + 1) * R_DEV])
            y = turns - ((turns + ROUND) - ROUND)
            at = 2 * p * LANES
            ph[z, :, at : at + LANES] = sine(0.25 - jnp.abs(y))
            ph[z, :, at + LANES : at + 2 * LANES] = sine(jnp.maximum(jnp.minimum(y, 0.5 - y), -0.5 - y))

    for b in range(EARLY_ROWS, 9):
        band_rows(b, unit)
    branch_rows(0)
    fill_phases(0)
    branch_rows(1)
    fill_phases(1)
    fill_phases(3)
    fill_phases(2)

    rest = wr.at[pl.ds(0, N_RP - 1)]
    pltpu.make_async_copy(rest, rest, w_recv.at[0]).wait()

    def both_parts(src, dst):
        for p in range(N_RP):
            re, im = src[p, 0], src[p, 1]
            dst[256 * p : 256 * p + 128, 0:128] = re
            dst[256 * p : 256 * p + 128, 128:256] = im
            dst[256 * p + 128 : 256 * p + 256, 0:128] = -im
            dst[256 * p + 128 : 256 * p + 256, 128:256] = re

    both_parts(wr, wx)

    @pl.when(is_hot)
    def _():
        rest = wr2.at[pl.ds(0, N_RP - 1)]
        pltpu.make_async_copy(rest, rest, w_recv.at[1]).wait()
        both_parts(wr2, wx2)

    me = rp * N_PB + pb

    mine = rp * N_NEAR + near

    def blocks_to(src, dst, sem, z, g):
        to_rp = lax.rem(rp + g, N_RP)

        def push(j):
            to_near = lax.rem(near + j, N_NEAR)
            pltpu.make_async_remote_copy(
                src(to_rp * N_NEAR + to_near), dst, f_send.at[sem], f_recv.at[sem],
                device_id=(to_rp, z * N_NEAR + to_near), device_id_type=MESH,
            ).start()

        @pl.when((to_rp != rp) | (z != far))
        def _():
            push(0)

        for j in range(1, N_NEAR):
            push(j)

    for d in NEXT:
        z = lax.rem(far + d, N_FAR)
        send[z, :, 0] = dot(ph[z], wx[...]).astype(BF16).reshape(64, 2, 256)

        @pl.when(is_hot)
        def _():
            send[z, :, 1] = dot(ph[z], wx2[...]).astype(BF16).reshape(64, 2, 256)

            @pl.loop(0, N_RP // 2)
            def _(g):
                for i in range(2):
                    blocks_to(lambda at: send.at[z, at], rv.at[me], 1, z, 2 * g + i)

        @pl.when(not_hot)
        def _():
            @pl.loop(0, N_RP // 2)
            def _(g):
                for i in range(2):
                    blocks_to(lambda at: send.at[z, at, 0], rv.at[me, 0], 0, z, 2 * g + i)

    rv[me, 0] = send[far, mine, 0]

    @pl.when(is_hot)
    def _():
        rv[me, 1] = send[far, mine, 1]

    def wait_pairs(count, sem):
        rest = rv.at[pl.ds(0, count)]
        pltpu.make_async_copy(rest, rest, sem).wait()

    def wait_blocks(count, sem):
        rest = rv.at[pl.ds(0, count), 0]
        pltpu.make_async_copy(rest, rest, sem).wait()

    @pl.when(is_hot)
    def _():
        wait_pairs(N_PB - 1, f_recv.at[1])
        wait_blocks(N_DEV - N_PB, f_recv.at[0])

    @pl.when(not_hot)
    def _():
        wait_pairs(N_PB, f_recv.at[1])
        wait_blocks(N_DEV - N_PB - 1, f_recv.at[0])

    for t in range(TILES):
        if t < N_RP:
            got = rv[t * N_PB : (t + 1) * N_PB, 0].reshape(2 * N_PB, 256)
        else:
            got = jnp.concatenate([rv[hot_rp(m) * N_PB + m : hot_rp(m) * N_PB + m + 1, 1] for m in range(N_PB)], axis=0)
            got = got.reshape(2 * N_PB, 256)
        part = dot(vb[...], got)
        re = (part[:64, :128] + part[64:, 128:]).astype(BF16)
        im = part[:64, 128:] - part[64:, :128]
        cols = slice(t * LANES, (t + 1) * LANES)
        more = slice(COLS + t * LANES, COLS + (t + 1) * LANES)
        y2[:64, cols] = re
        y2[64:, cols] = im.astype(BF16)
        y2[:64, more] = (-im).astype(BF16)
        y2[64:, more] = re
    for c0, width, _, _ in BANDS:
        part = dot(y2[...], ku[:, c0 : c0 + width])
        cols = slice(c0, c0 + width)
        for ql in range(2):
            re, im = part[32 * ql : 32 * ql + 32], part[64 + 32 * ql : 96 + 32 * ql]
            at = 64 * ql
            z2[0, at : at + 32, cols] = re.astype(BF16)
            z2[0, at + 32 : at + 64, cols] = im.astype(BF16)
            z2[1, at : at + 32, cols] = (-im).astype(BF16)
            z2[1, at + 32 : at + 64, cols] = re.astype(BF16)
    for ql in range(2):
        rows = slice(64 * ql, 64 * ql + 64)
        for t, (c0, width, r0, r1) in enumerate(BANDS):
            n = r1 - r0
            left = jnp.concatenate([z2[0, rows, r0:r1], z2[1, rows, r0:r1]], axis=1)
            out_ref[rows, c0 : c0 + width] = dot(left, ke[ql, t, 0 : 2 * n, 0:width])

    rest = q1.at[pl.ds(0, N_RP - 1)]
    pltpu.make_async_copy(rest, rest, q_send.at[0]).wait()
    rest = q2.at[pl.ds(0, N_PB - 1)]
    pltpu.make_async_copy(rest, rest, q_send.at[1]).wait()
    rest = wr.at[pl.ds(0, N_RP - 1)]
    pltpu.make_async_copy(rest, rest, w_send.at[0]).wait()

    @pl.when(is_hot)
    def _():
        wait_pairs(N_DEV - 1, f_send.at[1])

    @pl.when(not_hot)
    def _():
        wait_blocks(N_DEV - 1, f_send.at[0])
        pltpu.make_async_copy(wr.at[0], wr.at[0], w_send.at[1]).wait()


def local(wannier_g, rp_coords, q_coords, k_index, k_vectors, kq_vectors, modes):
    vmem = pl.BlockSpec(memory_space=pltpu.VMEM)
    smem = pl.BlockSpec(memory_space=pltpu.SMEM)
    hbm = pl.BlockSpec(memory_space=pltpu.HBM)
    out = pl.pallas_call(
        kernel,
        name="wannier_to_bloch",
        out_shape=pltpu.VMEM((4 * NB, COLS), F32),
        in_specs=[hbm, hbm, smem, smem, hbm, hbm, hbm],
        out_specs=vmem,
        scratch_shapes=[
            pltpu.VMEM((2, R_DEV, COLS), BF16),
            pltpu.VMEM((3, NR), jnp.int32),
            pltpu.VMEM(k_vectors.shape, BF16),
            pltpu.VMEM(kq_vectors.shape, BF16),
            pltpu.VMEM((2, NM, 2, NM), BF16),
            pltpu.VMEM((N_RP, 2, R_DEV, LANES), BF16),
            pltpu.VMEM((N_RP, 2, R_DEV, LANES), BF16),
            pltpu.VMEM((K_ALL, 256), BF16),
            pltpu.VMEM((K_ALL, 256), BF16),
            pltpu.VMEM((N_RP, 2, LANES), BF16),
            pltpu.VMEM((N_PB, 2, LANES), BF16),
            pltpu.VMEM((LANES, NR), BF16),
            pltpu.VMEM((N_FAR, 2 * N_RP * N_NEAR, K_ALL), BF16),
            pltpu.VMEM((N_FAR, N_RP * N_NEAR, 2, 2, 256), BF16),
            pltpu.VMEM((N_DEV, 2, 2, 256), BF16),
            pltpu.VMEM((128, 64), BF16),
            pltpu.VMEM((2 * COLS, COLS), BF16),
            pltpu.VMEM((2, 5, 1024, 256), BF16),
            pltpu.VMEM((128, 2 * COLS), BF16),
            pltpu.VMEM((2, 128, COLS), BF16),
            pltpu.SemaphoreType.DMA((5,)),
            pltpu.SemaphoreType.DMA((2,)),
            pltpu.SemaphoreType.DMA((5,)),
            pltpu.SemaphoreType.DMA((2,)),
            pltpu.SemaphoreType.DMA((2,)),
            pltpu.SemaphoreType.DMA((2,)),
            pltpu.SemaphoreType.DMA((2,)),
        ],
        compiler_params=pltpu.CompilerParams(
            collective_id=0, has_side_effects=True, vmem_limit_bytes=58 * 2**20
        ),
    )(wannier_g[:, :, 0, :], rp_coords, q_coords.T, k_index, k_vectors, kq_vectors, modes.transpose(0, 2, 1, 3))
    return out.reshape(2, 2, NB, COLS)


def solution(mesh):
    return jax.shard_map(
        local,
        mesh=mesh,
        in_specs=(
            P(None, "rp", "pb", None),
            P(),
            P(None, ("rp", "pb")),
            P(),
            P(),
            P(("rp", "pb"), None, None, None),
            P(("rp", "pb"), None, None, None),
        ),
        out_specs=P(("rp", "pb"), None, None, None),
        check_vma=False,
    )
```

```python
import functools
import math

import jax
import jax.numpy as jnp
from jax import lax
from jax.experimental import pallas as pl
from jax.experimental.pallas import tpu as pltpu
from jax.sharding import PartitionSpec as P

MESH = pl.DeviceIdType.MESH
F32 = jnp.float32
BF16 = jnp.bfloat16
NK = 16
N_RP = 8
N_PB = 32
N_FAR = 4
N_NEAR = 8
NEXT = (0, 1, 3, 2)
EARLY = ((1, 0), (0, 1), (3, 0), (1, 1), (3, 1))
LATE = ((2, 1), (2, 0))
ORDER = (2, 1, 3, 0)
EARLY_ROWS = 6
SINE = (6.281640231507743, -41.11355805211909, 73.72054790475445)
ROUND = 1.5 * 2.0**23
N_DEV = N_RP * N_PB
NB = 32
NM = 36
COLS = NB * NM
R_DEV = 128
LANES = 128
TILES = COLS // LANES
NR = R_DEV * N_RP
K_ALL = 2 * R_DEV * N_RP
BANDS = tuple(
    (256 * t, min(256, COLS - 256 * t), max(0, 256 * t - 128), min(COLS, 256 * t + 384)) for t in range(5)
)


def iota(shape, dim):
    return lax.broadcasted_iota(jnp.int32, shape, dim)


def band_of(x):
    return lax.shift_right_logical(x * 1821, 16)


def dot(a, b):
    return jnp.dot(a, b, preferred_element_type=F32)


def tdot(a, b):
    return lax.dot_general(a, b, (((0,), (0,)), ((), ())), preferred_element_type=F32)


def hot_rp(pb):
    far, y_at, core = pb // 8, pb % 8 // 2, pb % 2
    even = 2 * ((y_at + far) % 4) + (y_at + far // 2) % 2
    odd = (even + 4) % 8 + 1 - 2 * (even % 2)
    return even * (1 - core) + odd * core


def onehot(cond):
    return jnp.where(cond, 1.0, 0.0).astype(BF16)


def sine(c):
    c2 = c * c
    return (c * (SINE[0] + c2 * (SINE[1] + c2 * SINE[2]))).astype(BF16)


def kernel(
    w_hbm, rc_hbm, q_hbm, ki_hbm, kv_hbm, kq_hbm, e_hbm, out_ref,
    wv, rc, q_ref, ki_ref, kv, kq, em, wr, wr2, wx, wx2, q1, q2, ba, ph, send, rv, vb, ku, ke, y2, z2,
    in_sem, q_send, q_recv, w_send, w_recv, f_send, f_recv,
):
    rp, pb = lax.axis_index("rp"), lax.axis_index("pb")
    hot = hot_rp(pb)
    is_hot = rp == hot
    not_hot = rp != hot
    loads = [
        pltpu.make_async_copy(src, dst, in_sem.at[i])
        for i, (src, dst) in enumerate(
            (
                (q_hbm, q_ref),
                (ki_hbm, ki_ref),
                (w_hbm, wv),
                (rc_hbm, rc),
                (kv_hbm, kv),
                (kq_hbm, kq),
                (e_hbm, em),
            )
        )
    ]
    for load in loads:
        load.start()

    def w_peer(step):
        z = lax.rem(rp, 2)
        return 2 * lax.rem(rp // 2 + step[0], 4) + z + step[1] - 2 * z * step[1]

    far, near = pb // N_NEAR, lax.rem(pb, N_NEAR)
    x, z = rp // 2, lax.rem(rp, 2)
    flip = 1 - 2 * z
    flat_peers = [
        (2 * lax.rem(x + i, 4) + z, far * N_NEAR + lax.rem(near + j, N_NEAR))
        for i in range(4)
        for j in range(N_NEAR)
        if i + j
    ]
    deep_peers = [
        (d, (rp + f * flip, lax.rem(far + d, N_FAR) * N_NEAR + near)) for d in NEXT for f in range(2) if d + f
    ]
    other_peers = [(2 * lax.rem(x + i, 4) + z + flip, pb) for i in range(1, 4)]
    barrier = pltpu.get_barrier_semaphore()
    for other in flat_peers + [other for _, other in deep_peers] + other_peers:
        pl.semaphore_signal(barrier, inc=1, device_id=other, device_id_type=MESH)

    loads[0].wait()
    flat = x * N_NEAR + near
    lane, row = iota((8, LANES), 1), iota((8, LANES), 0)
    tile = jnp.zeros((8, LANES), F32)
    for ql in range(2):
        for axis in range(3):
            tile = tile + jnp.where((lane == 4 * flat + axis) & (row == ql), q_ref[ql, axis].astype(F32), 0.0)
    q1[flat] = tile[:2].astype(BF16)

    pl.semaphore_wait(barrier, len(flat_peers) + len(deep_peers) + len(other_peers))

    for other in flat_peers:
        pltpu.make_async_remote_copy(
            q1.at[flat], q1.at[flat], q_send.at[0], q_recv.at[0], device_id=other, device_id_type=MESH
        ).start()
    for load in loads[1:]:
        load.wait()

    def send_last():
        last = wv.at[:, :, pl.ds((TILES - 1) * LANES, LANES)]
        pltpu.make_async_remote_copy(
            last, wr2.at[rp], w_send.at[1], w_recv.at[1], device_id=(hot, pb), device_id_type=MESH
        ).start()

    def send_w(steps):
        for step in steps:
            other = 2 * lax.rem(x + step[0], 4) + z + step[1] * flip
            columns = pl.ds(pl.multiple_of(other * LANES, LANES), LANES)
            pltpu.make_async_remote_copy(
                wv.at[:, :, columns], wr.at[rp], w_send.at[0], w_recv.at[0], device_id=(other, pb), device_id_type=MESH
            ).start()

    @pl.when(not_hot)
    def _():
        send_last()

    send_w(EARLY)

    row = iota((16, NR), 0) % 4
    block = jnp.zeros((16, NR), F32)
    for axis in range(3):
        block = block + jnp.where(row == axis, rc[axis : axis + 1, :].astype(F32) / NK, 0.0)
    for g in range(LANES // 16):
        ba[16 * g : 16 * g + 16, :] = block.astype(BF16)

    wr[rp] = wv[:, :, pl.ds(pl.multiple_of(rp * LANES, LANES), LANES)]

    @pl.when(is_hot)
    def _():
        wr2[rp] = wv[:, :, pl.ds((TILES - 1) * LANES, LANES)]

    for ql in range(2):
        place = onehot(iota((NB, 2 * NB), 1) - 2 * iota((NB, 2 * NB), 0) == ql)
        for c in range(2):
            at = 64 * c + 32 * ql
            vb[at : at + 32] = tdot(kq[ql, c], place).astype(BF16)

    def band_rows(b, unit):
        spread = onehot(band_of(iota((NB, COLS), 1)) == iota((NB, COLS), 0))
        pick = onehot(band_of(b * LANES + iota((LANES, NB), 0)) == iota((LANES, NB), 1))
        r = b * LANES + iota((LANES, 1), 0)
        col = iota((1, COLS), 1)
        same = r - NM * band_of(r) == col - NM * band_of(col)
        for c in range(2):
            full = dot(dot(pick, unit[c]).astype(BF16), spread)
            ku[c * COLS + b * LANES : c * COLS + (b + 1) * LANES, :] = jnp.where(same, full, 0.0).astype(BF16)

    def branch_rows(ql):
        mode_col = iota((NM, COLS), 1)
        spread_m = onehot(mode_col - NM * band_of(mode_col) == iota((NM, COLS), 0))
        ec = dot(em[ql].reshape(2 * NM, NM), spread_m).astype(BF16)
        for t, (c0, width, r0, r1) in enumerate(BANDS):
            rows = r1 - r0
            r = r0 + iota((rows, 2 * NM), 0)
            at = iota((rows, 2 * NM), 1) - 2 * (r - NM * band_of(r))
            same = band_of(r0 + iota((rows, 1), 0)) == band_of(c0 + iota((1, width), 1))
            for c in range(2):
                full = dot(onehot(at == c), ec[:, c0 : c0 + width])
                ke[ql, t, c * rows : (c + 1) * rows, 0:width] = jnp.where(same, full, 0.0).astype(BF16)

    unit = kv[ki_ref[0]]
    for b in range(EARLY_ROWS):
        band_rows(b, unit)

    rest = q1.at[pl.ds(0, len(flat_peers))]
    pltpu.make_async_copy(rest, rest, q_recv.at[0]).wait()
    deep = 2 * far + z
    q2[deep] = jnp.sum(q1[...].astype(F32), axis=0).astype(BF16)
    for d, other in deep_peers:
        pltpu.make_async_remote_copy(
            q2.at[deep], q2.at[deep], q_send.at[1], q_recv.at[1 + (N_FAR - d) % N_FAR],
            device_id=other, device_id_type=MESH,
        ).start()
    send_w(LATE)

    def fill_phases(d):
        rest = q2.at[pl.ds(0, 2 - (d == 0))]
        pltpu.make_async_copy(rest, rest, q_recv.at[1 + d]).wait()
        group = lax.rem(far + d, N_FAR)
        row, lane = iota((LANES, LANES), 0), iota((LANES, LANES), 1)
        some = [q2[2 * group + i].astype(F32) for i in range(2)]
        row_of = [jnp.where(row % 2 == 0, some[i][0:1], some[i][1:2]) for i in range(2)]
        own = lane // 4 == row // 32 * N_NEAR + row // 2 % N_NEAR
        left = jnp.where(own, jnp.where(row // 16 % 2 == 0, row_of[0], row_of[1]), 0.0).astype(BF16)
        for p in range(N_RP):
            turns = dot(left, ba[:, p * R_DEV : (p + 1) * R_DEV])
            y = turns - ((turns + ROUND) - ROUND)
            at = 2 * p * LANES
            ph[group, :, at : at + LANES] = sine(0.25 - jnp.abs(y))
            ph[group, :, at + LANES : at + 2 * LANES] = sine(jnp.maximum(jnp.minimum(y, 0.5 - y), -0.5 - y))

    fill_phases(0)
    fill_phases(1)
    fill_phases(3)
    fill_phases(2)

    rest = wr.at[pl.ds(0, N_RP - 1)]
    pltpu.make_async_copy(rest, rest, w_recv.at[0]).wait()

    def both_parts(src, dst):
        for p in range(N_RP):
            re, im = src[p, 0], src[p, 1]
            dst[256 * p : 256 * p + 128, 0:128] = re
            dst[256 * p : 256 * p + 128, 128:256] = im
            dst[256 * p + 128 : 256 * p + 256, 0:128] = -im
            dst[256 * p + 128 : 256 * p + 256, 128:256] = re

    both_parts(wr, wx)

    @pl.when(is_hot)
    def _():
        rest = wr2.at[pl.ds(0, N_RP - 1)]
        pltpu.make_async_copy(rest, rest, w_recv.at[1]).wait()
        both_parts(wr2, wx2)

    me = rp * N_PB + pb

    mine = rp * N_NEAR + near

    def blocks_to(src, dst, sem, group, g):
        to_rp = lax.rem(rp + g, N_RP)

        def push(j):
            to_near = lax.rem(near + j, N_NEAR)
            pltpu.make_async_remote_copy(
                src(to_rp * N_NEAR + to_near), dst, f_send.at[sem], f_recv.at[sem],
                device_id=(to_rp, group * N_NEAR + to_near), device_id_type=MESH,
            ).start()

        @pl.when((to_rp != rp) | (group != far))
        def _():
            push(0)

        for j in range(1, N_NEAR):
            push(j)

    for d in ORDER:
        group = lax.rem(far + d, N_FAR)
        send[group, :, 0] = dot(ph[group], wx[...]).astype(BF16).reshape(64, 2, 256)

        @pl.when(is_hot)
        def _():
            send[group, :, 1] = dot(ph[group], wx2[...]).astype(BF16).reshape(64, 2, 256)

            @pl.loop(0, N_RP // 2)
            def _(g):
                for i in range(2):
                    blocks_to(lambda at: send.at[group, at], rv.at[me], 1, group, 2 * g + i)

        @pl.when(not_hot)
        def _():
            @pl.loop(0, N_RP // 2)
            def _(g):
                for i in range(2):
                    blocks_to(lambda at: send.at[group, at, 0], rv.at[me, 0], 0, group, 2 * g + i)

    rv[me, 0] = send[far, mine, 0]

    @pl.when(is_hot)
    def _():
        rv[me, 1] = send[far, mine, 1]

    for b in range(EARLY_ROWS, 9):
        band_rows(b, unit)
    branch_rows(0)
    branch_rows(1)

    def wait_pairs(count, sem):
        rest = rv.at[pl.ds(0, count)]
        pltpu.make_async_copy(rest, rest, sem).wait()

    def wait_blocks(count, sem):
        rest = rv.at[pl.ds(0, count), 0]
        pltpu.make_async_copy(rest, rest, sem).wait()

    @pl.when(is_hot)
    def _():
        wait_pairs(N_PB - 1, f_recv.at[1])
        wait_blocks(N_DEV - N_PB, f_recv.at[0])

    @pl.when(not_hot)
    def _():
        wait_pairs(N_PB, f_recv.at[1])
        wait_blocks(N_DEV - N_PB - 1, f_recv.at[0])

    for t in range(TILES):
        if t < N_RP:
            got = rv[t * N_PB : (t + 1) * N_PB, 0].reshape(2 * N_PB, 256)
        else:
            got = jnp.concatenate([rv[hot_rp(m) * N_PB + m : hot_rp(m) * N_PB + m + 1, 1] for m in range(N_PB)], axis=0)
            got = got.reshape(2 * N_PB, 256)
        part = dot(vb[...], got)
        re = (part[:64, :128] + part[64:, 128:]).astype(BF16)
        im = part[:64, 128:] - part[64:, :128]
        cols = slice(t * LANES, (t + 1) * LANES)
        more = slice(COLS + t * LANES, COLS + (t + 1) * LANES)
        y2[:64, cols] = re
        y2[64:, cols] = im.astype(BF16)
        y2[:64, more] = (-im).astype(BF16)
        y2[64:, more] = re
    for c0, width, _, _ in BANDS:
        part = dot(y2[...], ku[:, c0 : c0 + width])
        cols = slice(c0, c0 + width)
        for ql in range(2):
            re, im = part[32 * ql : 32 * ql + 32], part[64 + 32 * ql : 96 + 32 * ql]
            at = 64 * ql
            z2[0, at : at + 32, cols] = re.astype(BF16)
            z2[0, at + 32 : at + 64, cols] = im.astype(BF16)
            z2[1, at : at + 32, cols] = (-im).astype(BF16)
            z2[1, at + 32 : at + 64, cols] = re.astype(BF16)
    for ql in range(2):
        rows = slice(64 * ql, 64 * ql + 64)
        for t, (c0, width, r0, r1) in enumerate(BANDS):
            n = r1 - r0
            left = jnp.concatenate([z2[0, rows, r0:r1], z2[1, rows, r0:r1]], axis=1)
            out_ref[rows, c0 : c0 + width] = dot(left, ke[ql, t, 0 : 2 * n, 0:width])

    rest = q1.at[pl.ds(0, len(flat_peers))]
    pltpu.make_async_copy(rest, rest, q_send.at[0]).wait()
    rest = q2.at[pl.ds(0, len(deep_peers))]
    pltpu.make_async_copy(rest, rest, q_send.at[1]).wait()
    rest = wr.at[pl.ds(0, N_RP - 1)]
    pltpu.make_async_copy(rest, rest, w_send.at[0]).wait()

    @pl.when(is_hot)
    def _():
        wait_pairs(N_DEV - 1, f_send.at[1])

    @pl.when(not_hot)
    def _():
        wait_blocks(N_DEV - 1, f_send.at[0])
        pltpu.make_async_copy(wr.at[0], wr.at[0], w_send.at[1]).wait()


def local(wannier_g, rp_coords, q_coords, k_index, k_vectors, kq_vectors, modes):
    vmem = pl.BlockSpec(memory_space=pltpu.VMEM)
    hbm = pl.BlockSpec(memory_space=pltpu.HBM)
    out = pl.pallas_call(
        kernel,
        name="wannier_to_bloch",
        out_shape=pltpu.VMEM((4 * NB, COLS), F32),
        in_specs=[hbm] * 7,
        out_specs=vmem,
        scratch_shapes=[
            pltpu.VMEM((2, R_DEV, COLS), BF16),
            pltpu.VMEM((3, NR), jnp.int32),
            pltpu.SMEM((2, 3), jnp.int32),
            pltpu.SMEM((1,), jnp.int32),
            pltpu.VMEM(k_vectors.shape, BF16),
            pltpu.VMEM(kq_vectors.shape, BF16),
            pltpu.VMEM((2, NM, 2, NM), BF16),
            pltpu.VMEM((N_RP, 2, R_DEV, LANES), BF16),
            pltpu.VMEM((N_RP, 2, R_DEV, LANES), BF16),
            pltpu.VMEM((K_ALL, 256), BF16),
            pltpu.VMEM((K_ALL, 256), BF16),
            pltpu.VMEM((N_PB, 2, LANES), BF16),
            pltpu.VMEM((2 * N_FAR, 2, LANES), BF16),
            pltpu.VMEM((LANES, NR), BF16),
            pltpu.VMEM((N_FAR, 2 * N_RP * N_NEAR, K_ALL), BF16),
            pltpu.VMEM((N_FAR, N_RP * N_NEAR, 2, 2, 256), BF16),
            pltpu.VMEM((N_DEV, 2, 2, 256), BF16),
            pltpu.VMEM((128, 64), BF16),
            pltpu.VMEM((2 * COLS, COLS), BF16),
            pltpu.VMEM((2, 5, 1024, 256), BF16),
            pltpu.VMEM((128, 2 * COLS), BF16),
            pltpu.VMEM((2, 128, COLS), BF16),
            pltpu.SemaphoreType.DMA((7,)),
            pltpu.SemaphoreType.DMA((2,)),
            pltpu.SemaphoreType.DMA((5,)),
            pltpu.SemaphoreType.DMA((2,)),
            pltpu.SemaphoreType.DMA((2,)),
            pltpu.SemaphoreType.DMA((2,)),
            pltpu.SemaphoreType.DMA((2,)),
        ],
        compiler_params=pltpu.CompilerParams(
            collective_id=0, has_side_effects=True, vmem_limit_bytes=58 * 2**20
        ),
    )(wannier_g[:, :, 0, :], rp_coords, q_coords.T, k_index, k_vectors, kq_vectors, modes.transpose(0, 2, 1, 3))
    return out.reshape(2, 2, NB, COLS)


def solution(mesh):
    return jax.shard_map(
        local,
        mesh=mesh,
        in_specs=(
            P(None, "rp", "pb", None),
            P(),
            P(None, ("rp", "pb")),
            P(),
            P(),
            P(("rp", "pb"), None, None, None),
            P(("rp", "pb"), None, None, None),
        ),
        out_specs=P(("rp", "pb"), None, None, None),
        check_vma=False,
    )
```

```python
import functools
import math

import jax
import jax.numpy as jnp
from jax import lax
from jax.experimental import pallas as pl
from jax.experimental.pallas import tpu as pltpu
from jax.sharding import PartitionSpec as P

MESH = pl.DeviceIdType.MESH
F32 = jnp.float32
BF16 = jnp.bfloat16
NK = 16
N_RP = 8
N_PB = 32
N_FAR = 4
N_NEAR = 8
NEXT = (2, 1, 3, 0)
EARLY = ((1, 0), (0, 1), (3, 0), (1, 1), (3, 1))
LATE = ((2, 1), (2, 0))
EARLY_ROWS = 6
SINE = (6.281640231507743, -41.11355805211909, 73.72054790475445)
ROUND = 1.5 * 2.0**23
N_DEV = N_RP * N_PB
NB = 32
NM = 36
COLS = NB * NM
R_DEV = 128
LANES = 128
TILES = COLS // LANES
NR = R_DEV * N_RP
K_ALL = 2 * R_DEV * N_RP
BANDS = tuple(
    (256 * t, min(256, COLS - 256 * t), max(0, 256 * t - 128), min(COLS, 256 * t + 384)) for t in range(5)
)


def iota(shape, dim):
    return lax.broadcasted_iota(jnp.int32, shape, dim)


def band_of(x):
    return lax.shift_right_logical(x * 1821, 16)


def dot(a, b):
    return jnp.dot(a, b, preferred_element_type=F32)


def tdot(a, b):
    return lax.dot_general(a, b, (((0,), (0,)), ((), ())), preferred_element_type=F32)


def hot_rp(pb):
    far, y_at, core = pb // 8, pb % 8 // 2, pb % 2
    even = 2 * ((y_at + far) % 4) + (y_at + far // 2) % 2
    odd = (even + 4) % 8 + 1 - 2 * (even % 2)
    return even * (1 - core) + odd * core


def onehot(cond):
    return jnp.where(cond, 1.0, 0.0).astype(BF16)


def sine(c):
    c2 = c * c
    return (c * (SINE[0] + c2 * (SINE[1] + c2 * SINE[2]))).astype(BF16)


def kernel(
    w_hbm, rc_hbm, q_hbm, ki_hbm, kv_hbm, kq_hbm, e_hbm, out_ref,
    wv, rc, q_ref, ki_ref, kv, kq, em, wr, wr2, wx, q1, q2, ba, ph, send, rv, vb, ku, ke, y2, z2,
    in_sem, q_send, q_recv, w_send, w_recv, f_send, f_recv,
):
    rp, pb = lax.axis_index("rp"), lax.axis_index("pb")
    hot = hot_rp(pb)
    is_hot = rp == hot
    not_hot = rp != hot
    loads = [
        pltpu.make_async_copy(src, dst, in_sem.at[i])
        for i, (src, dst) in enumerate(
            (
                (q_hbm, q_ref),
                (ki_hbm, ki_ref),
                (w_hbm, wv),
                (rc_hbm, rc),
                (kv_hbm, kv),
                (kq_hbm, kq),
                (e_hbm, em),
            )
        )
    ]
    for load in loads:
        load.start()

    def w_peer(step):
        z = lax.rem(rp, 2)
        return 2 * lax.rem(rp // 2 + step[0], 4) + z + step[1] - 2 * z * step[1]

    far, near = pb // N_NEAR, lax.rem(pb, N_NEAR)
    x, z = rp // 2, lax.rem(rp, 2)
    flip = 1 - 2 * z
    flat_peers = [
        (2 * lax.rem(x + i, 4) + z, far * N_NEAR + lax.rem(near + j, N_NEAR))
        for i in (2, 1, 3, 0)
        for j in (4, 5, 2, 3, 6, 7, 1, 0)
        if i + j
    ]
    deep_peers = [
        (d, (rp + f * flip, lax.rem(far + d, N_FAR) * N_NEAR + near)) for d in NEXT for f in range(2) if d + f
    ]
    other_peers = [(2 * lax.rem(x + i, 4) + z + flip, pb) for i in range(1, 4)]
    barrier = pltpu.get_barrier_semaphore()
    for other in [other for _, other in deep_peers] + flat_peers + other_peers:
        pl.semaphore_signal(barrier, inc=1, device_id=other, device_id_type=MESH)

    loads[0].wait()
    flat = x * N_NEAR + near
    lane, row = iota((8, LANES), 1), iota((8, LANES), 0)
    tile = jnp.zeros((8, LANES), F32)
    for ql in range(2):
        for axis in range(3):
            tile = tile + jnp.where((lane == 4 * flat + axis) & (row == ql), q_ref[ql, axis].astype(F32), 0.0)
    q1[flat] = tile[:2].astype(BF16)

    pl.semaphore_wait(barrier, len(flat_peers) + len(deep_peers) + len(other_peers))

    for other in flat_peers:
        pltpu.make_async_remote_copy(
            q1.at[flat], q1.at[flat], q_send.at[0], q_recv.at[0], device_id=other, device_id_type=MESH
        ).start()
    for load in loads[1:]:
        load.wait()

    def send_last():
        last = wv.at[:, :, pl.ds((TILES - 1) * LANES, LANES)]
        pltpu.make_async_remote_copy(
            last, wr2.at[rp], w_send.at[1], w_recv.at[1], device_id=(hot, pb), device_id_type=MESH
        ).start()

    def send_w(steps):
        for step in steps:
            other = 2 * lax.rem(x + step[0], 4) + z + step[1] * flip
            columns = pl.ds(pl.multiple_of(other * LANES, LANES), LANES)
            pltpu.make_async_remote_copy(
                wv.at[:, :, columns], wr.at[rp], w_send.at[0], w_recv.at[0], device_id=(other, pb), device_id_type=MESH
            ).start()

    @pl.when(not_hot)
    def _():
        send_last()

    send_w(EARLY)

    row = iota((16, NR), 0) % 4
    block = jnp.zeros((16, NR), F32)
    for axis in range(3):
        block = block + jnp.where(row == axis, rc[axis : axis + 1, :].astype(F32) / NK, 0.0)
    for g in range(LANES // 16):
        ba[16 * g : 16 * g + 16, :] = block.astype(BF16)

    wr[rp] = wv[:, :, pl.ds(pl.multiple_of(rp * LANES, LANES), LANES)]

    @pl.when(is_hot)
    def _():
        wr2[rp] = wv[:, :, pl.ds((TILES - 1) * LANES, LANES)]

    for ql in range(2):
        place = onehot(iota((NB, 2 * NB), 1) - 2 * iota((NB, 2 * NB), 0) == ql)
        for c in range(2):
            at = 64 * c + 32 * ql
            vb[at : at + 32] = tdot(kq[ql, c], place).astype(BF16)

    def band_rows(b, unit):
        spread = onehot(band_of(iota((NB, COLS), 1)) == iota((NB, COLS), 0))
        pick = onehot(band_of(b * LANES + iota((LANES, NB), 0)) == iota((LANES, NB), 1))
        r = b * LANES + iota((LANES, 1), 0)
        col = iota((1, COLS), 1)
        same = r - NM * band_of(r) == col - NM * band_of(col)
        for c in range(2):
            full = dot(dot(pick, unit[c]).astype(BF16), spread)
            ku[c * COLS + b * LANES : c * COLS + (b + 1) * LANES, :] = jnp.where(same, full, 0.0).astype(BF16)

    def branch_rows(ql):
        mode_col = iota((NM, COLS), 1)
        spread_m = onehot(mode_col - NM * band_of(mode_col) == iota((NM, COLS), 0))
        ec = dot(em[ql].reshape(2 * NM, NM), spread_m).astype(BF16)
        for t, (c0, width, r0, r1) in enumerate(BANDS):
            rows = r1 - r0
            r = r0 + iota((rows, 2 * NM), 0)
            at = iota((rows, 2 * NM), 1) - 2 * (r - NM * band_of(r))
            same = band_of(r0 + iota((rows, 1), 0)) == band_of(c0 + iota((1, width), 1))
            for c in range(2):
                full = dot(onehot(at == c), ec[:, c0 : c0 + width])
                ke[ql, t, c * rows : (c + 1) * rows, 0:width] = jnp.where(same, full, 0.0).astype(BF16)

    unit = kv[ki_ref[0]]
    for b in range(EARLY_ROWS):
        band_rows(b, unit)

    rest = q1.at[pl.ds(0, len(flat_peers))]
    pltpu.make_async_copy(rest, rest, q_recv.at[0]).wait()
    deep = 2 * far + z
    q2[deep] = jnp.sum(q1[...].astype(F32), axis=0).astype(BF16)
    for d, other in deep_peers:
        pltpu.make_async_remote_copy(
            q2.at[deep], q2.at[deep], q_send.at[1], q_recv.at[1 + (N_FAR - d) % N_FAR],
            device_id=other, device_id_type=MESH,
        ).start()
    send_w(LATE)

    def fill_phases(d):
        rest = q2.at[pl.ds(0, 2 - (d == 0))]
        pltpu.make_async_copy(rest, rest, q_recv.at[1 + d]).wait()
        group = lax.rem(far + d, N_FAR)
        row, lane = iota((LANES, LANES), 0), iota((LANES, LANES), 1)
        some = [q2[2 * group + i].astype(F32) for i in range(2)]
        row_of = [jnp.where(row % 2 == 0, some[i][0:1], some[i][1:2]) for i in range(2)]
        own = lane // 4 == row // 32 * N_NEAR + row // 2 % N_NEAR
        left = jnp.where(own, jnp.where(row // 16 % 2 == 0, row_of[0], row_of[1]), 0.0).astype(BF16)
        for p in range(N_RP):
            turns = dot(left, ba[:, p * R_DEV : (p + 1) * R_DEV])
            y = turns - ((turns + ROUND) - ROUND)
            at = 2 * p * LANES
            ph[group, :, at : at + LANES] = sine(0.25 - jnp.abs(y))
            ph[group, :, at + LANES : at + 2 * LANES] = sine(jnp.maximum(jnp.minimum(y, 0.5 - y), -0.5 - y))

    fill_phases(0)
    fill_phases(1)
    fill_phases(3)
    fill_phases(2)

    rest = wr.at[pl.ds(0, N_RP - 1)]
    pltpu.make_async_copy(rest, rest, w_recv.at[0]).wait()

    def both_parts(src, at):
        for p in range(N_RP):
            re, im = src[p, 0], src[p, 1]
            wx[256 * p : 256 * p + 128, at : at + 128] = re
            wx[256 * p : 256 * p + 128, at + 128 : at + 256] = im
            wx[256 * p + 128 : 256 * p + 256, at : at + 128] = -im
            wx[256 * p + 128 : 256 * p + 256, at + 128 : at + 256] = re

    both_parts(wr, 0)

    @pl.when(is_hot)
    def _():
        rest = wr2.at[pl.ds(0, N_RP - 1)]
        pltpu.make_async_copy(rest, rest, w_recv.at[1]).wait()
        both_parts(wr2, 256)

    me = rp * N_PB + pb

    mine = rp * N_NEAR + near

    def blocks_to(src, dst, sem, group, g):
        to_rp = lax.rem(rp + g, N_RP)

        def push(j):
            to_near = lax.rem(near + j, N_NEAR)
            pltpu.make_async_remote_copy(
                src(to_rp * N_NEAR + to_near), dst, f_send.at[sem], f_recv.at[sem],
                device_id=(to_rp, group * N_NEAR + to_near), device_id_type=MESH,
            ).start()

        @pl.when((to_rp != rp) | (group != far))
        def _():
            push(0)

        for j in range(1, N_NEAR):
            push(j)

    for d in (2, 1 + 2 * z, 3 - 2 * z, 0):
        group = lax.rem(far + d, N_FAR)
        @pl.when(is_hot)
        def _():
            part = dot(ph[group], wx[...]).astype(BF16)
            for slot in range(2):
                send[group, :, slot] = part[:, 256 * slot : 256 * slot + 256].reshape(64, 2, 256)

            @pl.loop(0, N_RP // 2)
            def _(g):
                for i in range(2):
                    blocks_to(lambda at: send.at[group, at], rv.at[me], 1, group, 2 * g + i)

        @pl.when(not_hot)
        def _():
            send[group, :, 0] = dot(ph[group], wx[:, 0:256]).astype(BF16).reshape(64, 2, 256)

            @pl.loop(0, N_RP // 2)
            def _(g):
                for i in range(2):
                    blocks_to(lambda at: send.at[group, at, 0], rv.at[me, 0], 0, group, 2 * g + i)

    rv[me, 0] = send[far, mine, 0]

    @pl.when(is_hot)
    def _():
        rv[me, 1] = send[far, mine, 1]

    for b in range(EARLY_ROWS, 9):
        band_rows(b, unit)
    branch_rows(0)
    branch_rows(1)

    def wait_pairs(count, sem):
        rest = rv.at[pl.ds(0, count)]
        pltpu.make_async_copy(rest, rest, sem).wait()

    def wait_blocks(count, sem):
        rest = rv.at[pl.ds(0, count), 0]
        pltpu.make_async_copy(rest, rest, sem).wait()

    @pl.when(is_hot)
    def _():
        wait_pairs(N_PB - 1, f_recv.at[1])
        wait_blocks(N_DEV - N_PB, f_recv.at[0])

    @pl.when(not_hot)
    def _():
        wait_pairs(N_PB, f_recv.at[1])
        wait_blocks(N_DEV - N_PB - 1, f_recv.at[0])

    for t in range(TILES):
        if t < N_RP:
            got = rv[t * N_PB : (t + 1) * N_PB, 0].reshape(2 * N_PB, 256)
        else:
            got = jnp.concatenate([rv[hot_rp(m) * N_PB + m : hot_rp(m) * N_PB + m + 1, 1] for m in range(N_PB)], axis=0)
            got = got.reshape(2 * N_PB, 256)
        part = dot(vb[...], got)
        re = (part[:64, :128] + part[64:, 128:]).astype(BF16)
        im = part[:64, 128:] - part[64:, :128]
        cols = slice(t * LANES, (t + 1) * LANES)
        more = slice(COLS + t * LANES, COLS + (t + 1) * LANES)
        y2[:64, cols] = re
        y2[64:, cols] = im.astype(BF16)
        y2[:64, more] = (-im).astype(BF16)
        y2[64:, more] = re
    for c0, width, _, _ in BANDS:
        part = dot(y2[...], ku[:, c0 : c0 + width])
        cols = slice(c0, c0 + width)
        for ql in range(2):
            re, im = part[32 * ql : 32 * ql + 32], part[64 + 32 * ql : 96 + 32 * ql]
            at = 64 * ql
            z2[0, at : at + 32, cols] = re.astype(BF16)
            z2[0, at + 32 : at + 64, cols] = im.astype(BF16)
            z2[1, at : at + 32, cols] = (-im).astype(BF16)
            z2[1, at + 32 : at + 64, cols] = re.astype(BF16)
    for ql in range(2):
        rows = slice(64 * ql, 64 * ql + 64)
        for t, (c0, width, r0, r1) in enumerate(BANDS):
            n = r1 - r0
            left = jnp.concatenate([z2[0, rows, r0:r1], z2[1, rows, r0:r1]], axis=1)
            out_ref[rows, c0 : c0 + width] = dot(left, ke[ql, t, 0 : 2 * n, 0:width])

    rest = q1.at[pl.ds(0, len(flat_peers))]
    pltpu.make_async_copy(rest, rest, q_send.at[0]).wait()
    rest = q2.at[pl.ds(0, len(deep_peers))]
    pltpu.make_async_copy(rest, rest, q_send.at[1]).wait()
    rest = wr.at[pl.ds(0, N_RP - 1)]
    pltpu.make_async_copy(rest, rest, w_send.at[0]).wait()

    @pl.when(is_hot)
    def _():
        wait_pairs(N_DEV - 1, f_send.at[1])

    @pl.when(not_hot)
    def _():
        wait_blocks(N_DEV - 1, f_send.at[0])
        pltpu.make_async_copy(wr.at[0], wr.at[0], w_send.at[1]).wait()


def local(wannier_g, rp_coords, q_coords, k_index, k_vectors, kq_vectors, modes):
    vmem = pl.BlockSpec(memory_space=pltpu.VMEM)
    hbm = pl.BlockSpec(memory_space=pltpu.HBM)
    out = pl.pallas_call(
        kernel,
        name="wannier_to_bloch",
        out_shape=pltpu.VMEM((4 * NB, COLS), F32),
        in_specs=[hbm] * 7,
        out_specs=vmem,
        scratch_shapes=[
            pltpu.VMEM((2, R_DEV, COLS), BF16),
            pltpu.VMEM((3, NR), jnp.int32),
            pltpu.SMEM((2, 3), jnp.int32),
            pltpu.SMEM((1,), jnp.int32),
            pltpu.VMEM(k_vectors.shape, BF16),
            pltpu.VMEM(kq_vectors.shape, BF16),
            pltpu.VMEM((2, NM, 2, NM), BF16),
            pltpu.VMEM((N_RP, 2, R_DEV, LANES), BF16),
            pltpu.VMEM((N_RP, 2, R_DEV, LANES), BF16),
            pltpu.VMEM((K_ALL, 512), BF16),
            pltpu.VMEM((N_PB, 2, LANES), BF16),
            pltpu.VMEM((2 * N_FAR, 2, LANES), BF16),
            pltpu.VMEM((LANES, NR), BF16),
            pltpu.VMEM((N_FAR, 2 * N_RP * N_NEAR, K_ALL), BF16),
            pltpu.VMEM((N_FAR, N_RP * N_NEAR, 2, 2, 256), BF16),
            pltpu.VMEM((N_DEV, 2, 2, 256), BF16),
            pltpu.VMEM((128, 64), BF16),
            pltpu.VMEM((2 * COLS, COLS), BF16),
            pltpu.VMEM((2, 5, 1024, 256), BF16),
            pltpu.VMEM((128, 2 * COLS), BF16),
            pltpu.VMEM((2, 128, COLS), BF16),
            pltpu.SemaphoreType.DMA((7,)),
            pltpu.SemaphoreType.DMA((2,)),
            pltpu.SemaphoreType.DMA((5,)),
            pltpu.SemaphoreType.DMA((2,)),
            pltpu.SemaphoreType.DMA((2,)),
            pltpu.SemaphoreType.DMA((2,)),
            pltpu.SemaphoreType.DMA((2,)),
        ],
        compiler_params=pltpu.CompilerParams(
            collective_id=0, has_side_effects=True, vmem_limit_bytes=58 * 2**20
        ),
    )(wannier_g[:, :, 0, :], rp_coords, q_coords.T, k_index, k_vectors, kq_vectors, modes.transpose(0, 2, 1, 3))
    return out.reshape(2, 2, NB, COLS)


def solution(mesh):
    return jax.shard_map(
        local,
        mesh=mesh,
        in_specs=(
            P(None, "rp", "pb", None),
            P(),
            P(None, ("rp", "pb")),
            P(),
            P(),
            P(("rp", "pb"), None, None, None),
            P(("rp", "pb"), None, None, None),
        ),
        out_specs=P(("rp", "pb"), None, None, None),
        check_vma=False,
    )
```

```python
import functools
import math

import jax
import jax.numpy as jnp
from jax import lax
from jax.experimental import pallas as pl
from jax.experimental.pallas import tpu as pltpu
from jax.sharding import PartitionSpec as P

MESH = pl.DeviceIdType.MESH
F32 = jnp.float32
BF16 = jnp.bfloat16
NK = 16
N_RP = 8
N_PB = 32
N_FAR = 4
N_NEAR = 8
NEXT = (2, 1, 3, 0)
EARLY = ((1, 0), (0, 1), (3, 0), (1, 1), (3, 1))
LATE = ((2, 1), (2, 0))
EARLY_ROWS = 5
SINE = (6.281640231507743, -41.11355805211909, 73.72054790475445)
ROUND = 1.5 * 2.0**23
N_DEV = N_RP * N_PB
NB = 32
NM = 36
COLS = NB * NM
R_DEV = 128
LANES = 128
TILES = COLS // LANES
NR = R_DEV * N_RP
K_ALL = 2 * R_DEV * N_RP
BANDS = tuple(
    (256 * t, min(256, COLS - 256 * t), max(0, 256 * t - 128), min(COLS, 256 * t + 384)) for t in range(5)
)


def iota(shape, dim):
    return lax.broadcasted_iota(jnp.int32, shape, dim)


def band_of(x):
    return lax.shift_right_logical(x * 1821, 16)


def dot(a, b):
    return jnp.dot(a, b, preferred_element_type=F32)


def tdot(a, b):
    return lax.dot_general(a, b, (((0,), (0,)), ((), ())), preferred_element_type=F32)


def hot_rp(pb):
    far, y_at, core = pb // 8, pb % 8 // 2, pb % 2
    even = 2 * ((y_at + far) % 4) + (y_at + far // 2) % 2
    odd = (even + 4) % 8 + 1 - 2 * (even % 2)
    return even * (1 - core) + odd * core


def onehot(cond):
    return jnp.where(cond, 1.0, 0.0).astype(BF16)


def sine(c):
    c2 = c * c
    return (c * (SINE[0] + c2 * (SINE[1] + c2 * SINE[2]))).astype(BF16)


def kernel(
    w_hbm, rc_hbm, q_hbm, ki_hbm, kv_hbm, kq_hbm, e_hbm, out_ref,
    wv, rc, q_ref, ki_ref, kv, kq, em, wr, wr2, wx, q1, q2, ba, ph, send, rv, vb, ku, ke, y2, z2,
    in_sem, q_send, q_recv, w_send, w_recv, f_send, f_recv,
):
    rp, pb = lax.axis_index("rp"), lax.axis_index("pb")
    hot = hot_rp(pb)
    is_hot = rp == hot
    not_hot = rp != hot
    loads = [
        pltpu.make_async_copy(src, dst, in_sem.at[i])
        for i, (src, dst) in enumerate(
            (
                (q_hbm, q_ref),
                (ki_hbm, ki_ref),
                (w_hbm, wv),
                (rc_hbm, rc),
                (kv_hbm, kv),
                (kq_hbm, kq),
                (e_hbm, em),
            )
        )
    ]
    for load in loads:
        load.start()

    def w_peer(step):
        z = lax.rem(rp, 2)
        return 2 * lax.rem(rp // 2 + step[0], 4) + z + step[1] - 2 * z * step[1]

    far, near = pb // N_NEAR, lax.rem(pb, N_NEAR)
    x, z = rp // 2, lax.rem(rp, 2)
    flip = 1 - 2 * z
    flat_peers = [
        (2 * lax.rem(x + i, 4) + z, far * N_NEAR + lax.rem(near + j, N_NEAR))
        for i in (2, 1, 3, 0)
        for j in (4, 5, 2, 3, 6, 7, 1, 0)
        if i + j
    ]
    deep_peers = [
        (d, (rp + f * flip, lax.rem(far + d, N_FAR) * N_NEAR + near)) for d in NEXT for f in range(2) if d + f
    ]
    other_peers = [(2 * lax.rem(x + i, 4) + z + flip, pb) for i in range(1, 4)]
    barrier = pltpu.get_barrier_semaphore()
    for other in [other for _, other in deep_peers] + flat_peers + other_peers:
        pl.semaphore_signal(barrier, inc=1, device_id=other, device_id_type=MESH)

    loads[0].wait()
    flat = x * N_NEAR + near
    lane, row = iota((8, LANES), 1), iota((8, LANES), 0)
    tile = jnp.zeros((8, LANES), F32)
    for ql in range(2):
        for axis in range(3):
            tile = tile + jnp.where((lane == 4 * flat + axis) & (row == ql), q_ref[ql, axis].astype(F32), 0.0)
    q1[flat] = tile[:2].astype(BF16)

    pl.semaphore_wait(barrier, len(flat_peers) + len(deep_peers) + len(other_peers))

    for other in flat_peers:
        pltpu.make_async_remote_copy(
            q1.at[flat], q1.at[flat], q_send.at[0], q_recv.at[0], device_id=other, device_id_type=MESH
        ).start()
    for load in loads[1:]:
        load.wait()

    def send_last():
        last = wv.at[:, :, pl.ds((TILES - 1) * LANES, LANES)]
        pltpu.make_async_remote_copy(
            last, wr2.at[rp], w_send.at[1], w_recv.at[1], device_id=(hot, pb), device_id_type=MESH
        ).start()

    def send_w(steps):
        for step in steps:
            other = 2 * lax.rem(x + step[0], 4) + z + step[1] * flip
            columns = pl.ds(pl.multiple_of(other * LANES, LANES), LANES)
            pltpu.make_async_remote_copy(
                wv.at[:, :, columns], wr.at[rp], w_send.at[0], w_recv.at[0], device_id=(other, pb), device_id_type=MESH
            ).start()

    @pl.when(not_hot)
    def _():
        send_last()

    send_w(EARLY)

    row = iota((16, NR), 0) % 4
    block = jnp.zeros((16, NR), F32)
    for axis in range(3):
        block = block + jnp.where(row == axis, rc[axis : axis + 1, :].astype(F32) / NK, 0.0)
    for g in range(LANES // 16):
        ba[16 * g : 16 * g + 16, :] = block.astype(BF16)

    wr[rp] = wv[:, :, pl.ds(pl.multiple_of(rp * LANES, LANES), LANES)]

    @pl.when(is_hot)
    def _():
        wr2[rp] = wv[:, :, pl.ds((TILES - 1) * LANES, LANES)]

    for ql in range(2):
        place = onehot(iota((NB, 2 * NB), 1) - 2 * iota((NB, 2 * NB), 0) == ql)
        for c in range(2):
            at = 64 * c + 32 * ql
            vb[at : at + 32] = tdot(kq[ql, c], place).astype(BF16)

    def band_rows(b, unit):
        spread = onehot(band_of(iota((NB, COLS), 1)) == iota((NB, COLS), 0))
        pick = onehot(band_of(b * LANES + iota((LANES, NB), 0)) == iota((LANES, NB), 1))
        r = b * LANES + iota((LANES, 1), 0)
        col = iota((1, COLS), 1)
        same = r - NM * band_of(r) == col - NM * band_of(col)
        for c in range(2):
            full = dot(dot(pick, unit[c]).astype(BF16), spread)
            ku[c * COLS + b * LANES : c * COLS + (b + 1) * LANES, :] = jnp.where(same, full, 0.0).astype(BF16)

    def branch_rows(ql):
        mode_col = iota((NM, COLS), 1)
        spread_m = onehot(mode_col - NM * band_of(mode_col) == iota((NM, COLS), 0))
        ec = dot(em[ql].reshape(2 * NM, NM), spread_m).astype(BF16)
        for t, (c0, width, r0, r1) in enumerate(BANDS):
            rows = r1 - r0
            r = r0 + iota((rows, 2 * NM), 0)
            at = iota((rows, 2 * NM), 1) - 2 * (r - NM * band_of(r))
            same = band_of(r0 + iota((rows, 1), 0)) == band_of(c0 + iota((1, width), 1))
            for c in range(2):
                full = dot(onehot(at == c), ec[:, c0 : c0 + width])
                ke[ql, t, c * rows : (c + 1) * rows, 0:width] = jnp.where(same, full, 0.0).astype(BF16)

    unit = kv[ki_ref[0]]
    for b in range(EARLY_ROWS):
        band_rows(b, unit)

    rest = q1.at[pl.ds(0, len(flat_peers))]
    pltpu.make_async_copy(rest, rest, q_recv.at[0]).wait()
    deep = 2 * far + z
    q2[deep] = jnp.sum(q1[...].astype(F32), axis=0).astype(BF16)
    for d, other in deep_peers:
        pltpu.make_async_remote_copy(
            q2.at[deep], q2.at[deep], q_send.at[1], q_recv.at[1 + (N_FAR - d) % N_FAR],
            device_id=other, device_id_type=MESH,
        ).start()
    send_w(LATE)

    def fill_phases(d):
        rest = q2.at[pl.ds(0, 2 - (d == 0))]
        pltpu.make_async_copy(rest, rest, q_recv.at[1 + d]).wait()
        group = lax.rem(far + d, N_FAR)
        row, lane = iota((LANES, LANES), 0), iota((LANES, LANES), 1)
        some = [q2[2 * group + i].astype(F32) for i in range(2)]
        row_of = [jnp.where(row % 2 == 0, some[i][0:1], some[i][1:2]) for i in range(2)]
        own = lane // 4 == row // 32 * N_NEAR + row // 2 % N_NEAR
        left = jnp.where(own, jnp.where(row // 16 % 2 == 0, row_of[0], row_of[1]), 0.0).astype(BF16)
        for p in range(N_RP):
            turns = dot(left, ba[:, p * R_DEV : (p + 1) * R_DEV])
            y = turns - ((turns + ROUND) - ROUND)
            at = 2 * p * LANES
            ph[group, :, at : at + LANES] = sine(0.25 - jnp.abs(y))
            ph[group, :, at + LANES : at + 2 * LANES] = sine(jnp.maximum(jnp.minimum(y, 0.5 - y), -0.5 - y))

    fill_phases(0)
    fill_phases(1)
    fill_phases(3)
    fill_phases(2)

    rest = wr.at[pl.ds(0, N_RP - 1)]
    pltpu.make_async_copy(rest, rest, w_recv.at[0]).wait()

    def both_parts(src, at):
        for p in range(N_RP):
            re, im = src[p, 0], src[p, 1]
            wx[256 * p : 256 * p + 128, at : at + 128] = re
            wx[256 * p : 256 * p + 128, at + 128 : at + 256] = im
            wx[256 * p + 128 : 256 * p + 256, at : at + 128] = -im
            wx[256 * p + 128 : 256 * p + 256, at + 128 : at + 256] = re

    both_parts(wr, 0)

    @pl.when(is_hot)
    def _():
        rest = wr2.at[pl.ds(0, N_RP - 1)]
        pltpu.make_async_copy(rest, rest, w_recv.at[1]).wait()
        both_parts(wr2, 256)

    me = rp * N_PB + pb

    mine = rp * N_NEAR + near

    def blocks_to(src, dst, sem, group, g):
        to_rp = lax.rem(rp + g, N_RP)

        def push(j):
            to_near = lax.rem(near + j, N_NEAR)
            pltpu.make_async_remote_copy(
                src(to_rp * N_NEAR + to_near), dst, f_send.at[sem], f_recv.at[sem],
                device_id=(to_rp, group * N_NEAR + to_near), device_id_type=MESH,
            ).start()

        for j in (4, 5, 2, 3, 6, 7, 1):
            push(j)

        @pl.when((to_rp != rp) | (group != far))
        def _():
            push(0)

    odd = lax.rem(near // 2 + x + z, 2)
    for d in (2, 1 + 2 * odd, 3 - 2 * odd, 0):
        group = lax.rem(far + d, N_FAR)
        @pl.when(is_hot)
        def _():
            part = dot(ph[group], wx[...]).astype(BF16)
            for slot in range(2):
                send[group, :, slot] = part[:, 256 * slot : 256 * slot + 256].reshape(64, 2, 256)

            @pl.loop(0, N_RP // 2)
            def _(g):
                for i in range(2):
                    blocks_to(lambda at: send.at[group, at], rv.at[me], 1, group, 2 * g + i)

        @pl.when(not_hot)
        def _():
            send[group, :, 0] = dot(ph[group], wx[:, 0:256]).astype(BF16).reshape(64, 2, 256)

            @pl.loop(0, N_RP // 2)
            def _(g):
                for i in range(2):
                    blocks_to(lambda at: send.at[group, at, 0], rv.at[me, 0], 0, group, 2 * g + i)

    rv[me, 0] = send[far, mine, 0]

    @pl.when(is_hot)
    def _():
        rv[me, 1] = send[far, mine, 1]

    for b in range(EARLY_ROWS, 9):
        band_rows(b, unit)
    branch_rows(0)
    branch_rows(1)

    def wait_pairs(count, sem):
        rest = rv.at[pl.ds(0, count)]
        pltpu.make_async_copy(rest, rest, sem).wait()

    def wait_blocks(count, sem):
        rest = rv.at[pl.ds(0, count), 0]
        pltpu.make_async_copy(rest, rest, sem).wait()

    @pl.when(is_hot)
    def _():
        wait_pairs(N_PB - 1, f_recv.at[1])
        wait_blocks(N_DEV - N_PB, f_recv.at[0])

    @pl.when(not_hot)
    def _():
        wait_pairs(N_PB, f_recv.at[1])
        wait_blocks(N_DEV - N_PB - 1, f_recv.at[0])

    for t in range(TILES):
        if t < N_RP:
            got = rv[t * N_PB : (t + 1) * N_PB, 0].reshape(2 * N_PB, 256)
        else:
            got = jnp.concatenate([rv[hot_rp(m) * N_PB + m : hot_rp(m) * N_PB + m + 1, 1] for m in range(N_PB)], axis=0)
            got = got.reshape(2 * N_PB, 256)
        part = dot(vb[...], got)
        re = (part[:64, :128] + part[64:, 128:]).astype(BF16)
        im = part[:64, 128:] - part[64:, :128]
        cols = slice(t * LANES, (t + 1) * LANES)
        more = slice(COLS + t * LANES, COLS + (t + 1) * LANES)
        y2[:64, cols] = re
        y2[64:, cols] = im.astype(BF16)
        y2[:64, more] = (-im).astype(BF16)
        y2[64:, more] = re
    for c0, width, _, _ in BANDS:
        part = dot(y2[...], ku[:, c0 : c0 + width])
        cols = slice(c0, c0 + width)
        for ql in range(2):
            re, im = part[32 * ql : 32 * ql + 32], part[64 + 32 * ql : 96 + 32 * ql]
            at = 64 * ql
            z2[0, at : at + 32, cols] = re.astype(BF16)
            z2[0, at + 32 : at + 64, cols] = im.astype(BF16)
            z2[1, at : at + 32, cols] = (-im).astype(BF16)
            z2[1, at + 32 : at + 64, cols] = re.astype(BF16)
    for ql in range(2):
        rows = slice(64 * ql, 64 * ql + 64)
        for t, (c0, width, r0, r1) in enumerate(BANDS):
            n = r1 - r0
            left = jnp.concatenate([z2[0, rows, r0:r1], z2[1, rows, r0:r1]], axis=1)
            out_ref[rows, c0 : c0 + width] = dot(left, ke[ql, t, 0 : 2 * n, 0:width])

    rest = q1.at[pl.ds(0, len(flat_peers))]
    pltpu.make_async_copy(rest, rest, q_send.at[0]).wait()
    rest = q2.at[pl.ds(0, len(deep_peers))]
    pltpu.make_async_copy(rest, rest, q_send.at[1]).wait()
    rest = wr.at[pl.ds(0, N_RP - 1)]
    pltpu.make_async_copy(rest, rest, w_send.at[0]).wait()

    @pl.when(is_hot)
    def _():
        wait_pairs(N_DEV - 1, f_send.at[1])

    @pl.when(not_hot)
    def _():
        wait_blocks(N_DEV - 1, f_send.at[0])
        pltpu.make_async_copy(wr.at[0], wr.at[0], w_send.at[1]).wait()


def local(wannier_g, rp_coords, q_coords, k_index, k_vectors, kq_vectors, modes):
    vmem = pl.BlockSpec(memory_space=pltpu.VMEM)
    hbm = pl.BlockSpec(memory_space=pltpu.HBM)
    out = pl.pallas_call(
        kernel,
        name="wannier_to_bloch",
        out_shape=pltpu.VMEM((4 * NB, COLS), F32),
        in_specs=[hbm] * 7,
        out_specs=vmem,
        scratch_shapes=[
            pltpu.VMEM((2, R_DEV, COLS), BF16),
            pltpu.VMEM((3, NR), jnp.int32),
            pltpu.SMEM((2, 3), jnp.int32),
            pltpu.SMEM((1,), jnp.int32),
            pltpu.VMEM(k_vectors.shape, BF16),
            pltpu.VMEM(kq_vectors.shape, BF16),
            pltpu.VMEM((2, NM, 2, NM), BF16),
            pltpu.VMEM((N_RP, 2, R_DEV, LANES), BF16),
            pltpu.VMEM((N_RP, 2, R_DEV, LANES), BF16),
            pltpu.VMEM((K_ALL, 512), BF16),
            pltpu.VMEM((N_PB, 2, LANES), BF16),
            pltpu.VMEM((2 * N_FAR, 2, LANES), BF16),
            pltpu.VMEM((LANES, NR), BF16),
            pltpu.VMEM((N_FAR, 2 * N_RP * N_NEAR, K_ALL), BF16),
            pltpu.VMEM((N_FAR, N_RP * N_NEAR, 2, 2, 256), BF16),
            pltpu.VMEM((N_DEV, 2, 2, 256), BF16),
            pltpu.VMEM((128, 64), BF16),
            pltpu.VMEM((2 * COLS, COLS), BF16),
            pltpu.VMEM((2, 5, 1024, 256), BF16),
            pltpu.VMEM((128, 2 * COLS), BF16),
            pltpu.VMEM((2, 128, COLS), BF16),
            pltpu.SemaphoreType.DMA((7,)),
            pltpu.SemaphoreType.DMA((2,)),
            pltpu.SemaphoreType.DMA((5,)),
            pltpu.SemaphoreType.DMA((2,)),
            pltpu.SemaphoreType.DMA((2,)),
            pltpu.SemaphoreType.DMA((2,)),
            pltpu.SemaphoreType.DMA((2,)),
        ],
        compiler_params=pltpu.CompilerParams(
            collective_id=0, has_side_effects=True, vmem_limit_bytes=58 * 2**20
        ),
    )(wannier_g[:, :, 0, :], rp_coords, q_coords.T, k_index, k_vectors, kq_vectors, modes.transpose(0, 2, 1, 3))
    return out.reshape(2, 2, NB, COLS)


def solution(mesh):
    return jax.shard_map(
        local,
        mesh=mesh,
        in_specs=(
            P(None, "rp", "pb", None),
            P(),
            P(None, ("rp", "pb")),
            P(),
            P(),
            P(("rp", "pb"), None, None, None),
            P(("rp", "pb"), None, None, None),
        ),
        out_specs=P(("rp", "pb"), None, None, None),
        check_vma=False,
    )
```
